32 devices in a mesh: tok: 16 (over z, y, core), lay: 2 (over x).
Axes of the slice: x: 2, y: 2, z: 4, core: 2. Of those that a mesh axis runs over, the one named last changes fastest.
Arguments:
- first_acts: bfloat16 [2, 4096, 5120], P('lay', 'tok'), may hold values from -40 to 40
- second_acts: bfloat16 [2, 4096, 5120], P('lay', 'tok'), may hold values from -40 to 40
Outputs:
- whitening: float32 [2, 2, 40, 128, 128], P(None, 'lay')
- similarity: float32 [2, 2, 40], P('lay')
The draws below stay inside these ranges and needn't reach their ends.
All inputs are finite; a program needn't handle non-finite values.
Results may differ from the reference program's by a relative error of at most 0.0003.
Values may be sent and summed in bfloat16 or wider, within the bound.
A program may use at most 128 MiB of HBM per device.

```python
import math
import jax
import jax.numpy as jnp
from jax import lax

HEADS = 40
HEAD_DIM = 128
D = 5120
ITERS = 6
LAYERS = 2
TOKENS = 4096


def residual_layers(key):
    row_position = jnp.arange(TOKENS, dtype=jnp.float32) / TOKENS
    row_jitter = jax.random.uniform(jax.random.fold_in(key, 11), (TOKENS,), jnp.float32, -0.35, 0.35)
    row_scale = jnp.exp(math.log(3.0) * row_position + row_jitter)
    mixing = jnp.eye(HEAD_DIM, dtype=jnp.float32) + 0.8 / math.sqrt(HEAD_DIM) * jax.random.normal(jax.random.fold_in(key, 12), (HEADS, HEAD_DIM, HEAD_DIM), jnp.float32)
    stream = jnp.zeros((TOKENS, D), jnp.float32)
    first_list = []
    second_list = []
    for layer_idx in range(LAYERS):
        layer_key = jax.random.fold_in(key, 1000 + layer_idx)
        update = jax.random.normal(jax.random.fold_in(layer_key, 1), (TOKENS, D), jnp.float32)
        noise_part = jax.random.normal(jax.random.fold_in(layer_key, 3), (TOKENS, D), jnp.float32)
        chan_low = 0.3
        chan_high = 3.0
        stream = 0.8 * stream + 0.6 * update
        mixed_stream = jnp.einsum('thi,hij->thj', stream.reshape(TOKENS, HEADS, HEAD_DIM), mixing, precision=lax.Precision.HIGHEST).reshape(TOKENS, D)
        chan_first = jnp.exp(jax.random.uniform(jax.random.fold_in(layer_key, 4), (D,), jnp.float32, math.log(chan_low), math.log(chan_high)))
        chan_second = chan_first * jnp.exp(jax.random.uniform(jax.random.fold_in(layer_key, 5), (D,), jnp.float32, -0.35, 0.35))
        offset_first = 0.8 * jax.random.normal(jax.random.fold_in(layer_key, 6), (D,), jnp.float32)
        offset_second = offset_first + 0.3 * jax.random.normal(jax.random.fold_in(layer_key, 7), (D,), jnp.float32)
        first_layer = row_scale[:, None] * (chan_first * mixed_stream + offset_first)
        second_layer = row_scale[:, None] * (chan_second * (0.75 * mixed_stream + 0.66 * noise_part) + offset_second)
        first_list.append(jnp.clip(first_layer, -40.0, 40.0))
        second_list.append(jnp.clip(second_layer, -40.0, 40.0))
    return (jnp.stack(first_list), jnp.stack(second_list))


def draw_first_acts(key, part):
    return residual_layers(key)[0].astype(jnp.bfloat16)


def draw_second_acts(key, part):
    return residual_layers(key)[1].astype(jnp.bfloat16)


def setup_inputs(seed: int = 0) -> dict:
    arg_keys = jax.random.split(jax.random.key(seed), 3)
    return {
        "first_acts": draw_first_acts(jax.random.fold_in(arg_keys[2], 71), 0),
        "second_acts": draw_second_acts(jax.random.fold_in(arg_keys[2], 71), 0),
    }


ridge_weight = 0.05
top_precision = lax.Precision.HIGHEST

def newton_whiten(matrices):
    unit_matrix = jnp.eye(HEAD_DIM, dtype=jnp.float32)
    scale_norm = jnp.sqrt(lax.optimization_barrier(jnp.sum(matrices * matrices, axis=(-2, -1), keepdims=True)))
    square_iter = matrices / scale_norm
    inverse_iter = jnp.broadcast_to(unit_matrix, matrices.shape)
    for sweep_index in range(ITERS):
        factor_iter = 1.5 * unit_matrix - 0.5 * jnp.matmul(inverse_iter, square_iter, precision=top_precision)
        square_iter = jnp.matmul(square_iter, factor_iter, precision=top_precision)
        inverse_iter = jnp.matmul(factor_iter, inverse_iter, precision=top_precision)
    return inverse_iter / jnp.sqrt(scale_norm)

def covariance(gram_total, col_sums, token_total):
    unit_matrix = jnp.eye(HEAD_DIM, dtype=jnp.float32)
    column_mean = col_sums / token_total
    return gram_total / token_total - column_mean[..., :, None] * column_mean[..., None, :] + ridge_weight * unit_matrix

def head_view(act_block):
    return act_block.astype(jnp.float32).reshape(TOKENS, HEADS, HEAD_DIM)

def reference(first_acts, second_acts):
    gram_list = []
    sums_list = []
    for checkpoint in (first_acts, second_acts):
        for layer_idx in range(LAYERS):
            viewed = head_view(checkpoint[layer_idx])
            gram_list.append(jnp.einsum('thi,thj->hij', viewed, viewed, precision=top_precision))
            sums_list.append(lax.optimization_barrier(jnp.sum(viewed, axis=0)))
    gram_total = jnp.stack(gram_list).reshape(2, LAYERS, HEADS, HEAD_DIM, HEAD_DIM)
    col_sums = jnp.stack(sums_list).reshape(2, LAYERS, HEADS, HEAD_DIM)
    whitening = newton_whiten(covariance(gram_total, col_sums, TOKENS))
    column_mean = col_sums / TOKENS
    rows_out = []
    for first_idx in range(LAYERS):
        view_first = head_view(first_acts[first_idx])
        row_items = []
        for second_idx in range(LAYERS):
            view_second = head_view(second_acts[second_idx])
            cross_cov = jnp.einsum('thi,thj->hij', view_first, view_second, precision=top_precision) / TOKENS
            cross_cov = cross_cov - column_mean[0, first_idx][:, :, None] * column_mean[1, second_idx][:, None, :]
            left_product = jnp.matmul(whitening[0, first_idx], cross_cov, precision=top_precision)
            whitened = jnp.matmul(left_product, whitening[1, second_idx], precision=top_precision)
            row_items.append(lax.optimization_barrier(jnp.sum(whitened * whitened, axis=(-2, -1))) / HEAD_DIM)
        rows_out.append(jnp.stack(row_items))
    return (whitening, jnp.stack(rows_out))
```

```python
import functools

import jax
import jax.numpy as jnp
from jax import lax
from jax.experimental import pallas as pl
from jax.experimental.pallas import tpu as pltpu
from jax.sharding import PartitionSpec as P

HEADS = 40
HEAD_DIM = 128
ITERS = 6
PAD = 8

ridge_weight = 0.05
VMEM_LIMIT = 54 * 1024 * 1024
MESH = pl.DeviceIdType.MESH
HI = lax.Precision.HIGHEST


def dot_tt(a, b, precision=None):
    return lax.dot_general(
        a, b, (((0,), (0,)), ((), ())), preferred_element_type=jnp.float32, precision=precision
    )


def mm(a, b):
    return jnp.dot(a, b, preferred_element_type=jnp.float32, precision=HI)


BLOCKS = HEAD_DIM // 8
KEPT = BLOCKS // 2 + 1
PACKED = 8 * KEPT


def lane_block():
    return lax.broadcasted_iota(jnp.int32, (8, HEAD_DIM), 1) // 8


def pack(a):
    lb = lane_block()
    xs = [a[8 * e : 8 * e + 8, :] for e in range(BLOCKS)]
    step = 1
    while step < BLOCKS:
        bit = (lb // step) % 2 == 1
        xs = [jnp.where(bit, xs[(e + step) % BLOCKS], xs[e]) for e in range(BLOCKS)]
        step *= 2
    return jnp.concatenate([xs[(-d) % BLOCKS] for d in range(KEPT)], axis=0)


def unpack(p):
    lb = lane_block()
    zero = jnp.zeros((8, HEAD_DIM), jnp.float32)
    ys = [zero] * BLOCKS
    for d in range(KEPT):
        ys[(-d) % BLOCKS] = p[8 * d : 8 * d + 8, :]
    step = 1
    while step < BLOCKS:
        bit = (lb // step) % 2 == 1
        ys = [jnp.where(bit, ys[(e - step) % BLOCKS], ys[e]) for e in range(BLOCKS)]
        step *= 2
    half = jnp.concatenate(ys, axis=0)
    rb = lax.broadcasted_iota(jnp.int32, (HEAD_DIM, HEAD_DIM), 0) // 8
    cb = lax.broadcasted_iota(jnp.int32, (HEAD_DIM, HEAD_DIM), 1) // 8
    return jnp.where((cb - rb + BLOCKS) % BLOCKS < KEPT, half, half.T)


def kernel(
    n, R, hp, token_total,
    x1h, x2h, out, simout,
    x1, x2, x2o, gp, gd, gy, gz, cp, cd, cy, cz, slab, wbuf, sbuf, yb, zb,
    l_s, x_s, x_r, gd_s, gd_r, gy_s, gy_r, gz_s, gz_r,
    cd_s, cd_r, cy_s, cy_r, cz_s, cz_r,
    p_s, p_r, q_s, q_r, az_s, az_r, ay_s, ay_r, ad_s, ad_r, ss_s, ss_r,
):
    me = lax.axis_index("tok")
    lay = lax.axis_index("lay")
    other = 1 - lay
    c = lax.rem(me, 2)
    y = lax.rem(me // 2, 2)
    z = me // 4
    yn = 1 - y
    rows = x1.shape[0]
    D = HEAD_DIM
    core_peer = z * 4 + y * 2 + (1 - c)
    y_peer = z * 4 + yn * 2 + c
    padded = R * 2 * hp != HEADS

    def z_peer(zt):
        return zt * 4 + y * 2 + c

    def rc(src, dst, s, r, tok, ly):
        return pltpu.make_async_remote_copy(
            src_ref=src, dst_ref=dst, send_sem=s, recv_sem=r,
            device_id=(tok, ly), device_id_type=MESH,
        )

    def zt_of(i):
        return lax.rem(z + 1 + i, R)

    barrier = pltpu.get_barrier_semaphore()
    for k in range(1, n):
        pl.semaphore_signal(barrier, inc=1, device_id=(lax.rem(me + k, n), lay), device_id_type=MESH)
    pl.semaphore_signal(barrier, inc=1, device_id=(me, other), device_id_type=MESH)

    parts = 1 if padded else 2 * R
    width = x1.shape[1] // parts

    def part_cols(p):
        if padded:
            return pl.ds(0, width)
        half = yn if p % 2 == 0 else y
        return pl.ds(pl.multiple_of((zt_of(p // 2) * 2 + half) * width, 128), width)

    order = list(range(0, parts, 2)) + list(range(1, parts, 2))
    loads = {}
    for p in order:
        cols = part_cols(p)
        for k, (src, dst) in enumerate(((x2h, x2), (x1h, x1))):
            d = pltpu.make_async_copy(src.at[:, cols], dst.at[:, cols], l_s.at[2 * p + k])
            d.start()
            loads[p, k] = d

    def x_send(p):
        cols = part_cols(p)
        return rc(x2.at[:, cols], x2o.at[:, cols], x_s.at[p], x_r.at[p], me, other)

    pl.semaphore_wait(barrier, n)
    for p in range(parts):
        loads[p, 0].wait()
        x_send(p).start()
    for p in range(parts):
        loads[p, 1].wait()

    def head_cols(zt, yy, j):
        h = (zt * 2 + yy) * hp + j
        if padded:
            h = jnp.minimum(h, HEADS - 1)
        return pl.ds(pl.multiple_of(h * D, D), D)

    ones = jnp.ones((PAD, rows), jnp.bfloat16)

    def gram_half(i, half):
        zt = zt_of(i)
        yy = yn if half == 0 else y
        for j in range(hp):
            cols = head_cols(zt, yy, j)
            for k, ref in enumerate((x1, x2)):
                v = ref[:, cols]
                gp[k, zt, yy, j, :PACKED, :] = pack(dot_tt(v, v))
                gp[k, zt, yy, j, PACKED:, :] = jnp.dot(ones, v, preferred_element_type=jnp.float32)
        g_d(i, half).start()

    def g_d(i, half):
        zt = zt_of(i)
        yy = yn if half == 0 else y
        return rc(gp.at[1 - c, zt, yy], gd.at[zt, yy], gd_s.at[half, i], gd_r.at[half, i], core_peer, lay)

    def g_y(i):
        zt = zt_of(i)
        return rc(gp.at[c, zt, yn], gy.at[zt], gy_s.at[i], gy_r.at[i], y_peer, lay)

    def g_z(i):
        zt = zt_of(i)
        return rc(gp.at[c, zt, y], gz.at[i], gz_s.at[i], gz_r.at[i], z_peer(zt), lay)

    def g_yph(i):
        zt = zt_of(i)
        g_d(i, 0).wait_recv()
        for j in range(hp):
            gp[c, zt, yn, j] = gp[c, zt, yn, j] + gd[zt, yn, j]
        g_y(i).start()

    def g_zph(i, last):
        zt = zt_of(i)
        g_d(i, 1).wait_recv()
        g_y(i).wait_recv()
        for j in range(hp):
            gp[c, zt, y, j] = gp[c, zt, y, j] + gd[zt, y, j] + gy[zt, j]
        if not last:
            g_z(i).start()

    def first_body(i, carry):
        gram_half(i, 0)

        @pl.when(i >= 1)
        def _():
            g_yph(i - 1)

        return carry

    def second_body(i, carry):
        gram_half(i, 1)

        @pl.when(i == 0)
        def _():
            g_yph(R - 1)

        return carry

    lax.fori_loop(0, R, first_body, 0)
    lax.fori_loop(0, R, second_body, 0)

    def c_d(k, i, half):
        zt = zt_of(i)
        yy = yn if half == 0 else y
        return rc(cp.at[k, zt, yy], cd.at[zt, yy], cd_s.at[half, i], cd_r.at[half, i], core_peer, lay)

    def c_y(k, i):
        zt = zt_of(i)
        return rc(cp.at[k, zt, yn], cy.at[zt], cy_s.at[i], cy_r.at[i], y_peer, lay)

    def c_z(k, i):
        zt = zt_of(i)
        return rc(cp.at[k, zt, y], cz.at[i], cz_s.at[i], cz_r.at[i], z_peer(zt), lay)

    def cross_half(k, i, half):
        zt = zt_of(i)
        yy = yn if half == 0 else y
        ref = x2 if k == 0 else x2o
        for j in range(hp):
            cols = head_cols(zt, yy, j)
            cp[k, zt, yy, j] = dot_tt(x1[:, cols], ref[:, cols])

        @pl.when(c == 1 - k)
        def _():
            c_d(k, i, half).start()

    def cross_y(k, i):
        @pl.when(c == k)
        def _():
            zt = zt_of(i)
            c_d(k, i, 0).wait_recv()
            for j in range(hp):
                cp[k, zt, yn, j] = cp[k, zt, yn, j] + cd[zt, yn, j]
            c_y(k, i).start()

    def cross_z(k, i):
        @pl.when(c == k)
        def _():
            zt = zt_of(i)
            c_d(k, i, 1).wait_recv()
            c_y(k, i).wait_recv()
            for j in range(hp):
                cp[k, zt, y, j] = cp[k, zt, y, j] + cd[zt, y, j] + cy[zt, j]
            c_z(k, i).start()

    def loop(body, lo, hi):
        def step(i, carry):
            body(i)
            return carry

        lax.fori_loop(lo, hi, step, 0)

    def cross_own(half):
        def body(i):
            cross_half(0, i, half)

        loop(body, 0, R)

    def cross_other(i):
        for half in range(2):
            p = 2 * i + half
            if p < parts:
                x_send(p).wait_recv()
            cross_half(1, i, half)

    cross_own(0)
    g_zph(0, R == 1)
    cross_own(1)
    loop(lambda i: cross_y(0, i), 0, R)
    for i in range(1, R):
        g_zph(i, i == R - 1)
    cross_other(0)
    cross_y(1, 0)
    cross_z(0, 0)

    for i in range(R - 1):
        g_z(i).wait_recv()

    eye = (
        lax.broadcasted_iota(jnp.int32, (D, D), 0) == lax.broadcasted_iota(jnp.int32, (D, D), 1)
    ).astype(jnp.float32)
    scales = []
    for j in range(hp):
        total = gp[c, z, y, j]
        for i in range(R - 1):
            total = total + gz[i, j]
        mean = total[PACKED:, :] / token_total
        slab[0, j, D:, :] = mean
        cov = unpack(total[:PACKED, :]) / token_total - dot_tt(mean, mean, HI) * (1.0 / PAD) + ridge_weight * eye
        norm2 = jnp.sum(jnp.sum(cov * cov, axis=1, keepdims=True), axis=0, keepdims=True)
        scale = jnp.sqrt(norm2)
        scales.append(scale)
        y0 = cov / scale
        f = 1.5 * eye - 0.5 * y0
        yb[j] = mm(y0, f)
        zb[j] = f

    def ns_body(t, carry):
        fs = [1.5 * eye - 0.5 * mm(zb[j], yb[j]) for j in range(hp)]
        for j in range(hp):
            yb[j] = mm(yb[j], fs[j])
            zb[j] = mm(fs[j], zb[j])
        return carry

    lax.fori_loop(1, ITERS - 1, ns_body, 0)
    for j in range(hp):
        f = 1.5 * eye - 0.5 * mm(zb[j], yb[j])
        w = mm(f, zb[j]) / jnp.sqrt(scales[j])
        slab[0, j, :D, :] = w
        wbuf[c, z, y, j] = pack(w)
        out[c, z, y, j] = w

    def up(d):
        block = wbuf.at[c, z - d, y]
        return rc(block, block, az_s.at[0, d], az_r.at[0, d], z_peer(z + 1), lay)

    def down(d):
        block = wbuf.at[c, z + d, y]
        return rc(block, block, az_s.at[1, d], az_r.at[1, d], z_peer(z - 1), lay)

    def from_below(d):
        block = wbuf.at[c, z - d, y]
        return rc(block, block, az_s.at[0, d - 1], az_r.at[0, d - 1], z_peer(z - 1), lay)

    def from_above(d):
        block = wbuf.at[c, z + d, y]
        return rc(block, block, az_s.at[1, d - 1], az_r.at[1, d - 1], z_peer(z + 1), lay)

    def a_y(zs):
        block = wbuf.at[c, zs, y]
        return rc(block, block, ay_s.at[zs], ay_r.at[zs], y_peer, lay)

    def a_y_in(zs):
        block = wbuf.at[c, zs, yn]
        return rc(block, block, ay_s.at[zs], ay_r.at[zs], y_peer, lay)

    def a_d(cc, zs, half):
        block = wbuf.at[cc, zs, yn if half == 0 else y]
        return rc(block, block, ad_s.at[half, zs], ad_r.at[half, zs], core_peer, lay)

    to_core = rc(slab.at[0], slab.at[1], p_s.at[0], p_r.at[0], core_peer, lay)
    to_lay = rc(slab.at[0], slab.at[2], q_s.at[0], q_r.at[0], me, other)

    def has_below(d):
        return z - d >= 0

    def has_above(d):
        return z + d < R

    def when(cond):
        return pl.when(cond)

    @when(has_above(1))
    def _():
        up(0).start()

    @when(has_below(1))
    def _():
        down(0).start()

    a_y(z).start()
    to_core.start()
    a_d(c, z, 1).start()

    @pl.when(c == 1)
    def _():
        to_lay.start()

    def gather_z(d):
        @when(has_below(d))
        def _():
            from_below(d).wait_recv()

            @when(has_above(1))
            def _():
                up(d).start()

            a_y(z - d).start()
            a_d(c, z - d, 1).start()

        @when(has_above(d))
        def _():
            from_above(d).wait_recv()

            @when(has_below(1))
            def _():
                down(d).start()

            a_y(z + d).start()
            a_d(c, z + d, 1).start()

    def expand(cc, zs, yy):
        for j in range(hp):
            out[cc, zs, yy, j] = unpack(wbuf[cc, zs, yy, j])

    def sides(d, body):
        if d == 0:
            body(z)
            return

        @when(has_below(d))
        def _():
            body(z - d)

        @when(has_above(d))
        def _():
            body(z + d)

    def expand_z(d):
        sides(d, lambda zs: expand(c, zs, y))

    def gather_y(d):
        def body(zs):
            a_y_in(zs).wait_recv()
            a_d(c, zs, 0).start()
            expand(c, zs, yn)

        sides(d, body)

    def gather_core(d, half):
        def body(zs):
            a_d(1 - c, zs, half).wait_recv()
            expand(1 - c, zs, yn if half == 0 else y)

        sides(d, body)

    group = (z * 2 + y) * hp
    lane = lax.broadcasted_iota(jnp.int32, sbuf.shape[1:], 1)

    def s_out(k):
        return rc(sbuf.at[me], sbuf.at[me], ss_s.at[k], ss_r.at[k], lax.rem(me + k, n), lay)

    def s_in(k):
        src = lax.rem(me + n - k, n)
        return rc(sbuf.at[src], sbuf.at[src], ss_s.at[k], ss_r.at[k], src, lay)

    def final(k):
        @pl.when(c == k)
        def _():
            c_d(k, R - 1, 1).wait_recv()
            c_y(k, R - 1).wait_recv()
            for i in range(R - 1):
                c_z(k, i).wait_recv()
            to_core.wait_recv()
            if k == 1:
                to_lay.wait_recv()
            tile = jnp.zeros(sbuf.shape[1:], jnp.float32)
            for j in range(hp):
                total = cp[k, z, y, j] + cd[z, y, j] + cy[z, j]
                for i in range(R - 1):
                    total = total + cz[i, j]
                left = slab[k, j]
                right = slab[1 + k, j]
                cross = total / token_total - dot_tt(left[D:, :], right[D:, :], HI) * (1.0 / PAD)
                white = mm(mm(left[:D, :], cross), right[:D, :])
                value = jnp.sum(jnp.sum(white * white, axis=1, keepdims=True), axis=0, keepdims=True) / HEAD_DIM
                tile = jnp.where(lane == group + j, value, tile)
            sbuf[me] = tile
            for q in range(1, n):
                s_out(q).start()

    todo = []
    for i in range(1, R - 1):
        todo.append(lambda i=i: cross_z(0, i))
    own_steps = todo

    for f in own_steps:
        f()
    for i in range(1, R):
        cross_other(i)
        gather_z(i)
        cross_y(1, i)
        cross_z(1, i - 1)
        expand_z(i)
        gather_y(i - 1)
        if i == R - 2 or R == 2:
            final(0)
        gather_core(i - 1, 1)
    gather_y(R - 1)
    final(1)
    gather_core(R - 1, 1)
    for d in range(R):
        gather_core(d, 0)

    for k in range(1, n):
        s_in(k).wait_recv()
    row0 = sbuf[0]
    row1 = sbuf[1]
    for i in range(2, n, 2):
        row0 = row0 + sbuf[i]
        row1 = row1 + sbuf[i + 1]
    sub = lax.broadcasted_iota(jnp.int32, row0.shape, 0)
    simout[...] = jnp.where(sub == lay, row0, row1)[:2, :HEADS]

    for p in range(parts):
        x_send(p).wait_send()
    for i in range(R):
        for half in range(2):
            g_d(i, half).wait_send()
            c_d(1 - c, i, half).wait_send()
        g_y(i).wait_send()
        c_y(c, i).wait_send()
        a_y(i).wait_send()
        for half in range(2):
            a_d(c, i, half).wait_send()
    for i in range(R - 1):
        g_z(i).wait_send()
        c_z(c, i).wait_send()
    for d in range(R - 1):
        @when(jnp.logical_and(has_below(d), has_above(1)))
        def _():
            up(d).wait_send()

        @when(jnp.logical_and(has_above(d), has_below(1)))
        def _():
            down(d).wait_send()

    to_core.wait_send()

    @pl.when(c == 1)
    def _():
        to_lay.wait_send()

    for k in range(1, n):
        s_out(k).wait_send()


def solution(mesh):
    n = mesh.shape["tok"]
    R = n // 4
    hp = -(-HEADS // (n // 2))
    D = HEAD_DIM
    E = PACKED + PAD
    parts = 1 if R * 2 * hp != HEADS else 2 * R

    def local(first_acts, second_acts):
        _, rows, width = first_acts.shape
        token_total = float(rows * n)
        f32 = jnp.float32
        bf16 = jnp.bfloat16
        dma = lambda *k: pltpu.SemaphoreType.DMA(tuple(max(q, 1) for q in k))
        out, sims = pl.pallas_call(
            functools.partial(kernel, n, R, hp, token_total),
            out_shape=(
                pltpu.VMEM((2, R, 2, hp, D, D), f32),
                pltpu.VMEM((2, HEADS), f32),
            ),
            in_specs=[pl.BlockSpec(memory_space=pltpu.MemorySpace.HBM)] * 2,
            out_specs=(
                pl.BlockSpec(memory_space=pltpu.VMEM),
                pl.BlockSpec(memory_space=pltpu.VMEM),
            ),
            scratch_shapes=[
                pltpu.VMEM((rows, width), bf16),
                pltpu.VMEM((rows, width), bf16),
                pltpu.VMEM((rows, width), bf16),
                pltpu.VMEM((2, R, 2, hp, E, D), f32),
                pltpu.VMEM((R, 2, hp, E, D), f32),
                pltpu.VMEM((R, hp, E, D), f32),
                pltpu.VMEM((R - 1, hp, E, D), f32),
                pltpu.VMEM((2, R, 2, hp, D, D), f32),
                pltpu.VMEM((R, 2, hp, D, D), f32),
                pltpu.VMEM((R, hp, D, D), f32),
                pltpu.VMEM((R - 1, hp, D, D), f32),
                pltpu.VMEM((3, hp, D + PAD, D), f32),
                pltpu.VMEM((2, R, 2, hp, PACKED, D), f32),
                pltpu.VMEM((n, 8, D), f32),
                pltpu.VMEM((hp, D, D), f32),
                pltpu.VMEM((hp, D, D), f32),
                dma(2 * parts), dma(parts), dma(parts),
                dma(2, R), dma(2, R), dma(R), dma(R), dma(R - 1), dma(R - 1),
                dma(2, R), dma(2, R), dma(R), dma(R), dma(R - 1), dma(R - 1),
                dma(1), dma(1), dma(1), dma(1),
                dma(2, R), dma(2, R), dma(R), dma(R), dma(2, R), dma(2, R),
                dma(n), dma(n),
            ],
            compiler_params=pltpu.CompilerParams(
                collective_id=0, has_side_effects=True, vmem_limit_bytes=VMEM_LIMIT
            ),
        )(first_acts[0], second_acts[0])
        whitening = out.reshape(2, R * 2 * hp, D, D)[:, None, :HEADS]
        return whitening, sims[None]

    in_specs = (P("lay", "tok", None), P("lay", "tok", None))
    out_specs = (P(None, "lay", None, None, None), P("lay", None, None))
    return jax.shard_map(local, mesh=mesh, in_specs=in_specs, out_specs=out_specs, check_vma=False)
```

```python
import functools

import jax
import jax.numpy as jnp
from jax import lax
from jax.experimental import pallas as pl
from jax.experimental.pallas import tpu as pltpu
from jax.sharding import PartitionSpec as P

HEADS = 40
HEAD_DIM = 128
ITERS = 6
PAD = 8

ridge_weight = 0.05
Z_FIRST = 2
VMEM_LIMIT = 54 * 1024 * 1024
MESH = pl.DeviceIdType.MESH
HI = lax.Precision.HIGHEST


def dot_tt(a, b, precision=None):
    return lax.dot_general(
        a, b, (((0,), (0,)), ((), ())), preferred_element_type=jnp.float32, precision=precision
    )


def mm(a, b):
    return jnp.dot(a, b, preferred_element_type=jnp.float32, precision=HI)


BLOCKS = HEAD_DIM // 8
KEPT = BLOCKS // 2 + 1
PACKED = 8 * KEPT


def lane_block():
    return lax.broadcasted_iota(jnp.int32, (8, HEAD_DIM), 1) // 8


def pack(a):
    lb = lane_block()
    xs = [a[8 * e : 8 * e + 8, :] for e in range(BLOCKS)]
    step = 1
    while step < BLOCKS:
        bit = (lb // step) % 2 == 1
        xs = [jnp.where(bit, xs[(e + step) % BLOCKS], xs[e]) for e in range(BLOCKS)]
        step *= 2
    return jnp.concatenate([xs[(-d) % BLOCKS] for d in range(KEPT)], axis=0)


def unpack(p):
    lb = lane_block()
    zero = jnp.zeros((8, HEAD_DIM), jnp.float32)
    ys = [zero] * BLOCKS
    for d in range(KEPT):
        ys[(-d) % BLOCKS] = p[8 * d : 8 * d + 8, :]
    step = 1
    while step < BLOCKS:
        bit = (lb // step) % 2 == 1
        ys = [jnp.where(bit, ys[(e - step) % BLOCKS], ys[e]) for e in range(BLOCKS)]
        step *= 2
    half = jnp.concatenate(ys, axis=0)
    rb = lax.broadcasted_iota(jnp.int32, (HEAD_DIM, HEAD_DIM), 0) // 8
    cb = lax.broadcasted_iota(jnp.int32, (HEAD_DIM, HEAD_DIM), 1) // 8
    return jnp.where((cb - rb + BLOCKS) % BLOCKS < KEPT, half, half.T)


def kernel(
    n, R, hp, zf, token_total,
    x1h, x2h, out, simout,
    x1, x2, x2o, gp, gd, gy, gz, cp, cd, cy, cz, cyf, czf, slab, wbuf, sbuf, yb, zb,
    l_s, x_s, x_r, gd_s, gd_r, gy_s, gy_r, gz_s, gz_r,
    cd_s, cd_r, cy_s, cy_r, cz_s, cz_r, fy_s, fy_r, fz_s, fz_r,
    p_s, p_r, q_s, q_r, az_s, az_r, ay_s, ay_r, ad_s, ad_r, ss_s, ss_r,
):
    me = lax.axis_index("tok")
    lay = lax.axis_index("lay")
    other = 1 - lay
    c = lax.rem(me, 2)
    y = lax.rem(me // 2, 2)
    z = me // 4
    yn = 1 - y
    rows = x1.shape[0]
    D = HEAD_DIM
    core_peer = z * 4 + y * 2 + (1 - c)
    y_peer = z * 4 + yn * 2 + c
    padded = R * 2 * hp != HEADS

    bits = [1 << t for t in range(R.bit_length() - 1)]

    def z_xor(o):
        total = 0
        for b in bits:
            zb = lax.rem(z // b, 2)
            ob = lax.rem(o // b, 2) if not isinstance(o, int) else o // b % 2
            total = total + b * (zb + ob - 2 * zb * ob)
        return total

    def z_peer(o):
        return z_xor(o) * 4 + y * 2 + c

    def terms_of(o):
        return [b for b in bits if o % (2 * b) == 0]

    def lowest(o):
        return next(b for b in bits if o // b % 2)

    def rc(src, dst, s, r, tok, ly):
        return pltpu.make_async_remote_copy(
            src_ref=src, dst_ref=dst, send_sem=s, recv_sem=r,
            device_id=(tok, ly), device_id_type=MESH,
        )

    def zt_of(i):
        return z_xor(R - 1 - i)

    barrier = pltpu.get_barrier_semaphore()
    for k in range(1, n):
        pl.semaphore_signal(barrier, inc=1, device_id=(lax.rem(me + k, n), lay), device_id_type=MESH)
    pl.semaphore_signal(barrier, inc=1, device_id=(me, other), device_id_type=MESH)

    parts = 1 if padded else 2 * R
    width = x1.shape[1] // parts

    def part_cols(p):
        if padded:
            return pl.ds(0, width)
        half = yn if p % 2 == 0 else y
        return pl.ds(pl.multiple_of((zt_of(p // 2) * 2 + half) * width, 128), width)

    order = list(range(0, parts, 2)) + list(range(1, parts, 2))
    loads = {}
    for p in order:
        cols = part_cols(p)
        for k, (src, dst) in enumerate(((x2h, x2), (x1h, x1))):
            d = pltpu.make_async_copy(src.at[:, cols], dst.at[:, cols], l_s.at[2 * p + k])
            d.start()
            loads[p, k] = d

    def x_send(p):
        cols = part_cols(p)
        return rc(x2.at[:, cols], x2o.at[:, cols], x_s.at[p], x_r.at[p], me, other)

    pl.semaphore_wait(barrier, n)
    for p in range(parts):
        loads[p, 0].wait()
        x_send(p).start()
    for p in range(parts):
        loads[p, 1].wait()

    def head_cols(zt, yy, j):
        h = (zt * 2 + yy) * hp + j
        if padded:
            h = jnp.minimum(h, HEADS - 1)
        return pl.ds(pl.multiple_of(h * D, D), D)

    ones = jnp.ones((PAD, rows), jnp.bfloat16)
    sub8 = lax.broadcasted_iota(jnp.int32, (PAD, D), 0)

    def gram_half(i, half):
        zt = zt_of(i)
        yy = yn if half == 0 else y
        sums = [jnp.zeros((PAD, D), jnp.float32)] * 2
        for j in range(hp):
            cols = head_cols(zt, yy, j)
            for k, ref in enumerate((x1, x2)):
                v = ref[:, cols]
                gp[k, zt, yy, j * PACKED : (j + 1) * PACKED, :] = pack(dot_tt(v, v))
                sums[k] = jnp.where(sub8 == j, jnp.dot(ones, v, preferred_element_type=jnp.float32), sums[k])
        for k in range(2):
            gp[k, zt, yy, hp * PACKED :, :] = sums[k]
        g_d(i, half).start()

    def g_d(i, half):
        zt = zt_of(i)
        yy = yn if half == 0 else y
        return rc(gp.at[1 - c, zt, yy], gd.at[zt, yy], gd_s.at[half, i], gd_r.at[half, i], core_peer, lay)

    def g_y(i):
        zt = zt_of(i)
        return rc(gp.at[c, zt, yn], gy.at[zt], gy_s.at[i], gy_r.at[i], y_peer, lay)

    def g_z(o, b):
        return rc(gp.at[c, z_xor(o), y], gz.at[o - 1], gz_s.at[o - 1], gz_r.at[o - 1], z_peer(b), lay)

    def g_yph(i):
        zt = zt_of(i)
        g_d(i, 0).wait_recv()
        gp[c, zt, yn] = gp[c, zt, yn] + gd[zt, yn]
        g_y(i).start()

    def g_zph(i):
        zt = zt_of(i)
        o = R - 1 - i
        g_d(i, 1).wait_recv()
        g_y(i).wait_recv()
        terms = terms_of(o) if o else []
        for b in terms:
            g_z(o + b, b).wait_recv()
        total = gp[c, zt, y] + gd[zt, y] + gy[zt]
        for b in terms:
            total = total + gz[o + b - 1]
        gp[c, zt, y] = total
        if o:
            g_z(o, lowest(o)).start()

    def first_body(i, carry):
        gram_half(i, 0)

        @pl.when(i >= 1)
        def _():
            g_yph(i - 1)

        return carry

    def second_body(i, carry):
        gram_half(i, 1)

        @pl.when(i == 0)
        def _():
            g_yph(R - 1)

        return carry

    lax.fori_loop(0, R, first_body, 0)
    lax.fori_loop(0, R, second_body, 0)

    def c_d(k, i, half):
        zt = zt_of(i)
        yy = yn if half == 0 else y
        return rc(cp.at[k, zt, yy], cd.at[zt, yy], cd_s.at[half, i], cd_r.at[half, i], core_peer, lay)

    def own_heads(k):
        return pl.ds(zf, hp - zf) if k == 0 else pl.ds(0, hp)

    def c_y(k, i):
        zt = zt_of(i)
        hs = own_heads(k)
        return rc(cp.at[k, zt, yn, hs], cy.at[zt, hs], cy_s.at[i], cy_r.at[i], y_peer, lay)

    def c_z(k, o, b):
        hs = own_heads(k)
        return rc(cp.at[k, z_xor(o), y, hs], cz.at[o - 1, hs], cz_s.at[o - 1], cz_r.at[o - 1], z_peer(b), lay)

    def f_z(o, b):
        return rc(
            cp.at[0, z_xor(o), :, pl.ds(0, zf)], czf.at[o - 1], fz_s.at[o - 1], fz_r.at[o - 1], z_peer(b), lay
        )

    def f_y():
        return rc(cp.at[0, z, yn, pl.ds(0, zf)], cyf, fy_s.at[0], fy_r.at[0], y_peer, lay)

    def first_z(i):
        @pl.when(c == 0)
        def _():
            o = R - 1 - i
            zt = zt_of(i)
            for b in terms_of(o):
                f_z(o + b, b).wait_recv()
            for half in range(2):
                for j in range(zf):
                    total = cp[0, zt, half, j]
                    for b in terms_of(o):
                        total = total + czf[o + b - 1, half, j]
                    cp[0, zt, half, j] = total
            if o:
                f_z(o, lowest(o)).start()
            else:
                f_y().start()

    def cross_half(k, i, half):
        zt = zt_of(i)
        yy = yn if half == 0 else y
        ref = x2 if k == 0 else x2o
        for j in range(hp):
            cols = head_cols(zt, yy, j)
            cp[k, zt, yy, j] = dot_tt(x1[:, cols], ref[:, cols])

        @pl.when(c == 1 - k)
        def _():
            c_d(k, i, half).start()

    def cross_y(k, i):
        @pl.when(c == k)
        def _():
            zt = zt_of(i)
            c_d(k, i, 0).wait_recv()
            for j in range(hp):
                cp[k, zt, yn, j] = cp[k, zt, yn, j] + cd[zt, yn, j]
            c_y(k, i).start()
            if k == 0:
                c_d(k, i, 1).wait_recv()
                for j in range(hp):
                    cp[k, zt, y, j] = cp[k, zt, y, j] + cd[zt, y, j]

    def cross_z(k, i):
        @pl.when(c == k)
        def _():
            zt = zt_of(i)
            o = R - 1 - i
            if k == 1:
                c_d(k, i, 1).wait_recv()
            c_y(k, i).wait_recv()
            terms = terms_of(o)
            for b in terms:
                c_z(k, o + b, b).wait_recv()
            for j in range(zf if k == 0 else 0, hp):
                total = cp[k, zt, y, j] + cy[zt, j]
                if k == 1:
                    total = total + cd[zt, y, j]
                for b in terms:
                    total = total + cz[o + b - 1, j]
                cp[k, zt, y, j] = total
            c_z(k, o, lowest(o)).start()

    def loop(body, lo, hi):
        def step(i, carry):
            body(i)
            return carry

        lax.fori_loop(lo, hi, step, 0)

    def cross_own(half):
        def body(i):
            cross_half(0, i, half)

        loop(body, 0, R)

    def cross_other(i, half):
        p = 2 * i + half
        if p < parts:
            x_send(p).wait_recv()
        cross_half(1, i, half)

    cross_own(0)
    cross_own(1)
    g_zph(0)
    loop(lambda i: cross_y(0, i), 0, R)
    first_z(0)
    for i in range(1, R - 1):
        g_zph(i)
    cross_other(0, 0)
    cross_other(0, 1)
    g_zph(R - 1)
    cross_y(1, 0)
    cross_z(0, 0)
    for i in range(1, R - 1):
        first_z(i)
    for b in bits:
        g_z(b, b).wait_recv()

    eye = (
        lax.broadcasted_iota(jnp.int32, (D, D), 0) == lax.broadcasted_iota(jnp.int32, (D, D), 1)
    ).astype(jnp.float32)
    scales = []
    tail = slice(hp * PACKED, hp * PACKED + PAD)
    col_sums = gp[c, z, y, tail, :]
    for b in bits:
        col_sums = col_sums + gz[b - 1, tail, :]
    for j in range(hp):
        at = slice(j * PACKED, (j + 1) * PACKED)
        total = gp[c, z, y, at, :]
        for b in bits:
            total = total + gz[b - 1, at, :]
        mean = jnp.where(sub8 == 0, col_sums[j : j + 1, :], 0.0) / token_total
        slab[0, j, D:, :] = mean
        cov = unpack(total) / token_total - dot_tt(mean, mean, HI) + ridge_weight * eye
        norm2 = jnp.sum(jnp.sum(cov * cov, axis=1, keepdims=True), axis=0, keepdims=True)
        scale = jnp.sqrt(norm2)
        scales.append(scale)
        y0 = cov / scale
        f = 1.5 * eye - 0.5 * y0
        yb[j] = mm(y0, f)
        zb[j] = f

    def ns_body(t, carry):
        fs = [1.5 * eye - 0.5 * mm(zb[j], yb[j]) for j in range(hp)]
        for j in range(hp):
            yb[j] = mm(yb[j], fs[j])
            zb[j] = mm(fs[j], zb[j])
        return carry

    lax.fori_loop(1, ITERS - 1, ns_body, 0)
    for j in range(hp):
        f = 1.5 * eye - 0.5 * mm(zb[j], yb[j])
        w = mm(f, zb[j]) / jnp.sqrt(scales[j])
        slab[0, j, :D, :] = w
        wbuf[c, z, y, j] = pack(w)
        out[c, z, y, j] = w

    def a_z(o, b):
        block = wbuf.at[c, z_xor(o), y]
        return rc(block, block, az_s.at[o + b], az_r.at[o + b], z_peer(b), lay)

    def a_z_in(o):
        block = wbuf.at[c, z_xor(o), y]
        return rc(block, block, az_s.at[o], az_r.at[o], z_peer(lowest(o)), lay)

    def a_y(o, half):
        block = wbuf.at[c, z_xor(o), yn if half == 0 else y]
        return rc(block, block, ay_s.at[o], ay_r.at[o], y_peer, lay)

    def a_d(cc, o, half):
        block = wbuf.at[cc, z_xor(o), yn if half == 0 else y]
        return rc(block, block, ad_s.at[half, o], ad_r.at[half, o], core_peer, lay)

    to_core = rc(slab.at[0], slab.at[1], p_s.at[0], p_r.at[0], core_peer, lay)
    to_lay = rc(slab.at[0], slab.at[2], q_s.at[0], q_r.at[0], me, other)

    def forward(o):
        for b in terms_of(o):
            a_z(o, b).start()
        a_y(o, 1).start()
        a_d(c, o, 1).start()

    def expand(cc, o, yy):
        zs = z_xor(o)
        for j in range(hp):
            out[cc, zs, yy, j] = unpack(wbuf[cc, zs, yy, j])

    def gather_z(o):
        a_z_in(o).wait_recv()
        forward(o)

    def expand_z(o):
        expand(c, o, y)

    def gather_y(o):
        a_y(o, 0).wait_recv()
        a_d(c, o, 0).start()
        expand(c, o, yn)

    def gather_core(o, half):
        a_d(1 - c, o, half).wait_recv()
        expand(1 - c, o, yn if half == 0 else y)

    forward(0)
    to_core.start()

    @pl.when(c == 1)
    def _():
        to_lay.start()

    group = (z * 2 + y) * hp
    lane = lax.broadcasted_iota(jnp.int32, sbuf.shape[1:], 1)

    def s_out(k):
        return rc(sbuf.at[me], sbuf.at[me], ss_s.at[k], ss_r.at[k], lax.rem(me + k, n), lay)

    def s_in(k):
        src = lax.rem(me + n - k, n)
        return rc(sbuf.at[src], sbuf.at[src], ss_s.at[k], ss_r.at[k], src, lay)

    def final(k):
        @pl.when(c == k)
        def _():
            if k == 0:
                f_y().wait_recv()
            else:
                c_d(k, R - 1, 1).wait_recv()
            c_y(k, R - 1).wait_recv()
            for b in bits:
                c_z(k, b, b).wait_recv()
            to_core.wait_recv()
            if k == 1:
                to_lay.wait_recv()
            tile = jnp.zeros(sbuf.shape[1:], jnp.float32)
            for j in range(hp):
                if k == 0 and j < zf:
                    total = cp[k, z, y, j] + cyf[j]
                else:
                    total = cp[k, z, y, j] + cy[z, j]
                    if k == 1:
                        total = total + cd[z, y, j]
                    for b in bits:
                        total = total + cz[b - 1, j]
                left = slab[k, j]
                right = slab[1 + k, j]
                cross = total / token_total - dot_tt(left[D:, :], right[D:, :], HI)
                white = mm(mm(left[:D, :], cross), right[:D, :])
                value = jnp.sum(jnp.sum(white * white, axis=1, keepdims=True), axis=0, keepdims=True) / HEAD_DIM
                tile = jnp.where(lane == group + j, value, tile)
            sbuf[me] = tile
            for q in range(1, n):
                s_out(q).start()

    for i in range(1, R - 1):
        cross_z(0, i)
    cross_z(1, 0)
    steps = sorted(range(1, R), key=lambda o: (bin(o).count("1"), o))
    lag = [0]
    seen = []
    for i in range(1, R - 1):
        new = steps[-(-(R - 1) * (i - 1) // (R - 2)) : -(-(R - 1) * i // (R - 2))]
        cross_other(i, 0)
        if i > 1:
            cross_z(1, i - 1)
        cross_other(i, 1)
        cross_y(1, i)
        if i == 1:
            first_z(R - 1)
        gather_z(new[0])
        for o in lag:
            gather_y(o)
        for o in new[1:]:
            gather_z(o)
        for o in new:
            expand_z(o)
        seen += lag
        lag = new
    final(0)
    cross_other(R - 1, 0)
    cross_z(1, R - 2)
    cross_y(1, R - 1)
    for o in seen:
        gather_core(o, 1)
    for o in lag:
        gather_y(o)
    cross_other(R - 1, 1)
    for o in lag:
        gather_core(o, 1)
    final(1)
    for o in seen + lag:
        gather_core(o, 0)

    for k in range(1, n):
        s_in(k).wait_recv()
    row0 = sbuf[0]
    row1 = sbuf[1]
    for i in range(2, n, 2):
        row0 = row0 + sbuf[i]
        row1 = row1 + sbuf[i + 1]
    sub = lax.broadcasted_iota(jnp.int32, row0.shape, 0)
    simout[...] = jnp.where(sub == lay, row0, row1)[:2, :HEADS]

    for p in range(parts):
        x_send(p).wait_send()
    for i in range(R):
        for half in range(2):
            g_d(i, half).wait_send()
            c_d(1 - c, i, half).wait_send()
        g_y(i).wait_send()
        for k in range(2):
            @pl.when(c == k)
            def _():
                c_y(k, i).wait_send()

        a_y(i, 1).wait_send()
        for half in range(2):
            a_d(c, i, half).wait_send()
    for o in range(R):
        if o:
            g_z(o, lowest(o)).wait_send()

            @pl.when(c == 0)
            def _():
                c_z(0, o, lowest(o)).wait_send()
                f_z(o, lowest(o)).wait_send()

            @pl.when(c == 1)
            def _():
                c_z(1, o, lowest(o)).wait_send()
        for b in bits:
            if b in terms_of(o):
                a_z(o, b).wait_send()

    to_core.wait_send()

    @pl.when(c == 0)
    def _():
        f_y().wait_send()

    @pl.when(c == 1)
    def _():
        to_lay.wait_send()

    for k in range(1, n):
        s_out(k).wait_send()


def solution(mesh):
    n = mesh.shape["tok"]
    R = n // 4
    hp = -(-HEADS // (n // 2))
    zf = max(hp * Z_FIRST // 5, 1)
    D = HEAD_DIM
    E = hp * PACKED + PAD
    parts = 1 if R * 2 * hp != HEADS else 2 * R

    def local(first_acts, second_acts):
        _, rows, width = first_acts.shape
        token_total = float(rows * n)
        f32 = jnp.float32
        bf16 = jnp.bfloat16
        dma = lambda *k: pltpu.SemaphoreType.DMA(tuple(max(q, 1) for q in k))
        out, sims = pl.pallas_call(
            functools.partial(kernel, n, R, hp, zf, token_total),
            out_shape=(
                pltpu.VMEM((2, R, 2, hp, D, D), f32),
                pltpu.VMEM((2, HEADS), f32),
            ),
            in_specs=[pl.BlockSpec(memory_space=pltpu.MemorySpace.HBM)] * 2,
            out_specs=(
                pl.BlockSpec(memory_space=pltpu.VMEM),
                pl.BlockSpec(memory_space=pltpu.VMEM),
            ),
            scratch_shapes=[
                pltpu.VMEM((rows, width), bf16),
                pltpu.VMEM((rows, width), bf16),
                pltpu.VMEM((rows, width), bf16),
                pltpu.VMEM((2, R, 2, E, D), f32),
                pltpu.VMEM((R, 2, E, D), f32),
                pltpu.VMEM((R, E, D), f32),
                pltpu.VMEM((R - 1, E, D), f32),
                pltpu.VMEM((2, R, 2, hp, D, D), f32),
                pltpu.VMEM((R, 2, hp, D, D), f32),
                pltpu.VMEM((R, hp, D, D), f32),
                pltpu.VMEM((R - 1, hp, D, D), f32),
                pltpu.VMEM((zf, D, D), f32),
                pltpu.VMEM((R - 1, 2, zf, D, D), f32),
                pltpu.VMEM((3, hp, D + PAD, D), f32),
                pltpu.VMEM((2, R, 2, hp, PACKED, D), f32),
                pltpu.VMEM((n, 8, D), f32),
                pltpu.VMEM((hp, D, D), f32),
                pltpu.VMEM((hp, D, D), f32),
                dma(2 * parts), dma(parts), dma(parts),
                dma(2, R), dma(2, R), dma(R), dma(R), dma(R - 1), dma(R - 1),
                dma(2, R), dma(2, R), dma(R), dma(R), dma(R - 1), dma(R - 1), dma(1), dma(1), dma(R - 1), dma(R - 1),
                dma(1), dma(1), dma(1), dma(1),
                dma(R), dma(R), dma(R), dma(R), dma(2, R), dma(2, R),
                dma(n), dma(n),
            ],
            compiler_params=pltpu.CompilerParams(
                collective_id=0, has_side_effects=True, vmem_limit_bytes=VMEM_LIMIT
            ),
        )(first_acts[0], second_acts[0])
        whitening = out.reshape(2, R * 2 * hp, D, D)[:, None, :HEADS]
        return whitening, sims[None]

    in_specs = (P("lay", "tok", None), P("lay", "tok", None))
    out_specs = (P(None, "lay", None, None, None), P("lay", None, None))
    return jax.shard_map(local, mesh=mesh, in_specs=in_specs, out_specs=out_specs, check_vma=False)
```

```python
import functools

import jax
import jax.numpy as jnp
from jax import lax
from jax.experimental import pallas as pl
from jax.experimental.pallas import tpu as pltpu
from jax.sharding import PartitionSpec as P

HEADS = 40
HEAD_DIM = 128
ITERS = 6
PAD = 8

ridge_weight = 0.05
Z_FIRST = 2
VMEM_LIMIT = 54 * 1024 * 1024
MESH = pl.DeviceIdType.MESH
HI = lax.Precision.HIGHEST


def dot_tt(a, b, precision=None):
    return lax.dot_general(
        a, b, (((0,), (0,)), ((), ())), preferred_element_type=jnp.float32, precision=precision
    )


def mm(a, b):
    return jnp.dot(a, b, preferred_element_type=jnp.float32, precision=HI)


BLOCKS = HEAD_DIM // 8
KEPT = BLOCKS // 2 + 1
PACKED = 8 * KEPT


def lane_block():
    return lax.broadcasted_iota(jnp.int32, (8, HEAD_DIM), 1) // 8


def pack(a):
    lb = lane_block()
    xs = [a[8 * e : 8 * e + 8, :] for e in range(BLOCKS)]
    step = 1
    while step < BLOCKS:
        bit = (lb // step) % 2 == 1
        xs = [jnp.where(bit, xs[(e + step) % BLOCKS], xs[e]) for e in range(BLOCKS)]
        step *= 2
    return jnp.concatenate([xs[(-d) % BLOCKS] for d in range(KEPT)], axis=0)


def unpack(p):
    lb = lane_block()
    zero = jnp.zeros((8, HEAD_DIM), jnp.float32)
    ys = [zero] * BLOCKS
    for d in range(KEPT):
        ys[(-d) % BLOCKS] = p[8 * d : 8 * d + 8, :]
    step = 1
    while step < BLOCKS:
        bit = (lb // step) % 2 == 1
        ys = [jnp.where(bit, ys[(e - step) % BLOCKS], ys[e]) for e in range(BLOCKS)]
        step *= 2
    half = jnp.concatenate(ys, axis=0)
    rb = lax.broadcasted_iota(jnp.int32, (HEAD_DIM, HEAD_DIM), 0) // 8
    cb = lax.broadcasted_iota(jnp.int32, (HEAD_DIM, HEAD_DIM), 1) // 8
    return jnp.where((cb - rb + BLOCKS) % BLOCKS < KEPT, half, half.T)


def kernel(
    n, R, hp, zf, token_total,
    x1h, x2h, out, simout,
    x1, x2, x2o, gp, gd, gy, gz, cp, cd, cy, cz, cyf, czf, slab, wbuf, sbuf, yb, zb,
    l_s, x_s, x_r, gd_s, gd_r, gy_s, gy_r, gz_s, gz_r,
    cd_s, cd_r, cy_s, cy_r, cz_s, cz_r, fy_s, fy_r, fz_s, fz_r,
    p_s, p_r, q_s, q_r, az_s, az_r, ay_s, ay_r, ad_s, ad_r, ss_s, ss_r,
):
    me = lax.axis_index("tok")
    lay = lax.axis_index("lay")
    other = 1 - lay
    c = lax.rem(me, 2)
    y = lax.rem(me // 2, 2)
    z = me // 4
    yn = 1 - y
    rows = x1.shape[0]
    D = HEAD_DIM
    core_peer = z * 4 + y * 2 + (1 - c)
    y_peer = z * 4 + yn * 2 + c
    padded = R * 2 * hp != HEADS

    bits = [1 << t for t in range(R.bit_length() - 1)]

    def z_xor(o):
        total = 0
        for b in bits:
            zb = lax.rem(z // b, 2)
            ob = lax.rem(o // b, 2) if not isinstance(o, int) else o // b % 2
            total = total + b * (zb + ob - 2 * zb * ob)
        return total

    def z_peer_at(zt):
        return zt * 4 + y * 2 + c

    def z_peer(o):
        return z_xor(o) * 4 + y * 2 + c

    def at_least(a, b):
        return (a - b + R) // R

    def ct_of(i):
        step = R - 1 - i
        below = z
        above = R - 1 - z
        short = jnp.minimum(below, above)
        up_far = at_least(above, below)
        paired = 1 - at_least(step, 2 * short + 1)
        dist = paired * ((step + 1) // 2) + (1 - paired) * (step - short)
        near_side = paired * (1 - lax.rem(step, 2))
        up = up_far + near_side - 2 * up_far * near_side
        return z + dist * (2 * up - 1)

    def hop(zt):
        return 2 * at_least(zt, z) - 1

    def slot_of(zt):
        direction = hop(zt)
        last = (R - direction * (zt - z)) // (R - 1)
        down = (1 - direction) // 2
        return zt + (R - zt) * last * down

    def has_source(zt):
        return inside(z - hop(zt))

    def inside(q):
        return at_least(q, 0) * at_least(R - 1, q)

    def terms_of(o):
        return [b for b in bits if o % (2 * b) == 0]

    def lowest(o):
        return next(b for b in bits if o // b % 2)

    def rc(src, dst, s, r, tok, ly):
        return pltpu.make_async_remote_copy(
            src_ref=src, dst_ref=dst, send_sem=s, recv_sem=r,
            device_id=(tok, ly), device_id_type=MESH,
        )

    def zt_of(i):
        return z_xor(R - 1 - i)

    barrier = pltpu.get_barrier_semaphore()
    for k in range(1, n):
        pl.semaphore_signal(barrier, inc=1, device_id=(lax.rem(me + k, n), lay), device_id_type=MESH)
    pl.semaphore_signal(barrier, inc=1, device_id=(me, other), device_id_type=MESH)

    parts = 1 if padded else 2 * R
    width = x1.shape[1] // parts

    def part_cols(p):
        if padded:
            return pl.ds(0, width)
        half = yn if p % 2 == 0 else y
        return pl.ds(pl.multiple_of((ct_of(p // 2) * 2 + half) * width, 128), width)

    order = list(range(0, parts, 2)) + list(range(1, parts, 2))
    loads = {}
    for p in order:
        cols = part_cols(p)
        for k, (src, dst) in enumerate(((x2h, x2), (x1h, x1))):
            d = pltpu.make_async_copy(src.at[:, cols], dst.at[:, cols], l_s.at[2 * p + k])
            d.start()
            loads[p, k] = d

    def x_send(p):
        cols = part_cols(p)
        return rc(x2.at[:, cols], x2o.at[:, cols], x_s.at[p], x_r.at[p], me, other)

    pl.semaphore_wait(barrier, n)
    for p in range(parts):
        loads[p, 0].wait()
        x_send(p).start()
    for p in range(parts):
        loads[p, 1].wait()

    def head_cols(zt, yy, j):
        h = (zt * 2 + yy) * hp + j
        if padded:
            h = jnp.minimum(h, HEADS - 1)
        return pl.ds(pl.multiple_of(h * D, D), D)

    ones = jnp.ones((PAD, rows), jnp.bfloat16)
    sub8 = lax.broadcasted_iota(jnp.int32, (PAD, D), 0)

    def gram_half(i, half):
        zt = zt_of(i)
        yy = yn if half == 0 else y
        sums = [jnp.zeros((PAD, D), jnp.float32)] * 2
        for j in range(hp):
            cols = head_cols(zt, yy, j)
            for k, ref in enumerate((x1, x2)):
                v = ref[:, cols]
                gp[k, zt, yy, j * PACKED : (j + 1) * PACKED, :] = pack(dot_tt(v, v))
                sums[k] = jnp.where(sub8 == j, jnp.dot(ones, v, preferred_element_type=jnp.float32), sums[k])
        for k in range(2):
            gp[k, zt, yy, hp * PACKED :, :] = sums[k]
        g_d(i, half).start()

    def g_d(i, half):
        zt = zt_of(i)
        yy = yn if half == 0 else y
        return rc(gp.at[1 - c, zt, yy], gd.at[zt, yy], gd_s.at[half, i], gd_r.at[half, i], core_peer, lay)

    def g_y(i):
        zt = zt_of(i)
        return rc(gp.at[c, zt, yn], gy.at[zt], gy_s.at[i], gy_r.at[i], y_peer, lay)

    def g_z(o, b):
        return rc(gp.at[c, z_xor(o), y], gz.at[o - 1], gz_s.at[o - 1], gz_r.at[o - 1], z_peer(b), lay)

    def g_yph(i):
        zt = zt_of(i)
        g_d(i, 0).wait_recv()
        gp[c, zt, yn] = gp[c, zt, yn] + gd[zt, yn]
        g_y(i).start()

    def g_zph(i):
        zt = zt_of(i)
        o = R - 1 - i
        g_d(i, 1).wait_recv()
        g_y(i).wait_recv()
        terms = terms_of(o) if o else []
        for b in terms:
            g_z(o + b, b).wait_recv()
        total = gp[c, zt, y] + gd[zt, y] + gy[zt]
        for b in terms:
            total = total + gz[o + b - 1]
        gp[c, zt, y] = total
        if o:
            g_z(o, lowest(o)).start()

    def first_body(i, carry):
        gram_half(i, 0)

        @pl.when(i >= 1)
        def _():
            g_yph(i - 1)

        return carry

    def second_body(i, carry):
        gram_half(i, 1)

        @pl.when(i == 0)
        def _():
            g_yph(R - 1)

        return carry

    lax.fori_loop(0, R, first_body, 0)

    def c_d(k, i, half):
        zt = ct_of(i)
        yy = yn if half == 0 else y
        return rc(cp.at[k, zt, yy], cd.at[zt, yy], cd_s.at[half, i], cd_r.at[half, i], core_peer, lay)

    def own_heads(k):
        return pl.ds(zf, hp - zf) if k == 0 else pl.ds(0, hp)

    def c_y(k, i):
        zt = ct_of(i)
        hs = own_heads(k)
        return rc(cp.at[k, zt, yn, hs], cy.at[zt, hs], cy_s.at[i], cy_r.at[i], y_peer, lay)

    def c_z(k, zt, slot):
        hs = own_heads(k)
        return rc(cp.at[k, zt, y, hs], cz.at[slot, hs], cz_s.at[zt], cz_r.at[slot], z_peer_at(z + hop(zt)), lay)

    def c_z_in(k, slot):
        hs = own_heads(k)
        return rc(cp.at[k, z, y, hs], cz.at[slot, hs], cz_s.at[z], cz_r.at[slot], me, other)

    def f_z(zt, slot):
        return rc(
            cp.at[0, zt, :, pl.ds(0, zf)], czf.at[slot], fz_s.at[zt], fz_r.at[slot], z_peer_at(z + hop(zt)), lay
        )

    def f_z_in(slot):
        return rc(cp.at[0, z, :, pl.ds(0, zf)], czf.at[slot], fz_s.at[z], fz_r.at[slot], me, other)

    def f_y():
        return rc(cp.at[0, z, yn, pl.ds(0, zf)], cyf, fy_s.at[0], fy_r.at[0], y_peer, lay)

    def sources(zt, own, body):
        if own:
            pl.when(z > 0)(lambda: body(z))
            pl.when(z < R - 1)(lambda: body(R))
        else:
            pl.when(has_source(zt) == 1)(lambda: body(zt))

    def first_z(i, chained=None):
        ready = c == 0
        if chained is not None:
            ready = jnp.logical_and(ready, has_source(ct_of(i)) == chained)

        @pl.when(ready)
        def _():
            own = i == R - 1
            zt = ct_of(i)

            def add(slot):
                f_z_in(slot).wait_recv()
                for half in range(2):
                    for j in range(zf):
                        cp[0, zt, half, j] = cp[0, zt, half, j] + czf[slot, half, j]

            sources(zt, own, add)
            if own:
                f_y().start()
            else:
                f_z(zt, slot_of(zt)).start()

    def cross_half(k, i, half):
        zt = ct_of(i)
        yy = yn if half == 0 else y
        ref = x2 if k == 0 else x2o
        for j in range(hp):
            cols = head_cols(zt, yy, j)
            cp[k, zt, yy, j] = dot_tt(x1[:, cols], ref[:, cols])

        @pl.when(c == 1 - k)
        def _():
            c_d(k, i, half).start()

    def cross_y(k, i):
        @pl.when(c == k)
        def _():
            zt = ct_of(i)
            c_d(k, i, 0).wait_recv()
            for j in range(hp):
                cp[k, zt, yn, j] = cp[k, zt, yn, j] + cd[zt, yn, j]
            c_y(k, i).start()
            if k == 0:
                c_d(k, i, 1).wait_recv()
                for j in range(hp):
                    cp[k, zt, y, j] = cp[k, zt, y, j] + cd[zt, y, j]

    def cross_z(k, i, chained):
        @pl.when(jnp.logical_and(c == k, has_source(ct_of(i)) == chained))
        def _():
            zt = ct_of(i)
            if k == 1:
                c_d(k, i, 1).wait_recv()
            c_y(k, i).wait_recv()
            for j in range(zf if k == 0 else 0, hp):
                total = cp[k, zt, y, j] + cy[zt, j]
                if k == 1:
                    total = total + cd[zt, y, j]
                cp[k, zt, y, j] = total

            def add(slot):
                c_z_in(k, slot).wait_recv()
                for j in range(zf if k == 0 else 0, hp):
                    cp[k, zt, y, j] = cp[k, zt, y, j] + cz[slot, j]

            sources(zt, False, add)
            c_z(k, zt, slot_of(zt)).start()

    def loop(body, lo, hi):
        def step(i, carry):
            body(i)
            return carry

        lax.fori_loop(lo, hi, step, 0)

    def cross_own(i):
        cross_half(0, i, 0)
        cross_half(0, i, 1)

    def cross_other(i, half):
        p = 2 * i + half
        if p < parts:
            x_send(p).wait_recv()
        cross_half(1, i, half)

    cross_own(0)
    lax.fori_loop(0, R, second_body, 0)
    cross_y(0, 0)
    first_z(0, 0)
    loop(cross_own, 1, R)
    g_zph(0)
    loop(lambda i: cross_y(0, i), 1, R)
    for i in range(1, R - 1):
        g_zph(i)
        if i == 1:
            first_z(0, 1)
            first_z(1, 0)
    cross_other(0, 0)
    cross_other(0, 1)
    g_zph(R - 1)
    cross_y(1, 0)
    for b in bits:
        g_z(b, b).wait_recv()

    eye = (
        lax.broadcasted_iota(jnp.int32, (D, D), 0) == lax.broadcasted_iota(jnp.int32, (D, D), 1)
    ).astype(jnp.float32)
    scales = []
    tail = slice(hp * PACKED, hp * PACKED + PAD)
    col_sums = gp[c, z, y, tail, :]
    for b in bits:
        col_sums = col_sums + gz[b - 1, tail, :]
    for j in range(hp):
        at = slice(j * PACKED, (j + 1) * PACKED)
        total = gp[c, z, y, at, :]
        for b in bits:
            total = total + gz[b - 1, at, :]
        mean = jnp.where(sub8 == 0, col_sums[j : j + 1, :], 0.0) / token_total
        slab[0, j, D:, :] = mean
        cov = unpack(total) / token_total - dot_tt(mean, mean, HI) + ridge_weight * eye
        norm2 = jnp.sum(jnp.sum(cov * cov, axis=1, keepdims=True), axis=0, keepdims=True)
        scale = jnp.sqrt(norm2)
        scales.append(scale)
        y0 = cov / scale
        f = 1.5 * eye - 0.5 * y0
        yb[j] = mm(y0, f)
        zb[j] = f

    def ns_body(t, carry):
        fs = [1.5 * eye - 0.5 * mm(zb[j], yb[j]) for j in range(hp)]
        for j in range(hp):
            yb[j] = mm(yb[j], fs[j])
            zb[j] = mm(fs[j], zb[j])
        return carry

    lax.fori_loop(1, ITERS - 1, ns_body, 0)
    for j in range(hp):
        f = 1.5 * eye - 0.5 * mm(zb[j], yb[j])
        w = mm(f, zb[j]) / jnp.sqrt(scales[j])
        slab[0, j, :D, :] = w
        wbuf[c, z, y, j] = pack(w)
        out[c, z, y, j] = w

    def up(d):
        block = wbuf.at[c, z - d, y]
        return rc(block, block, az_s.at[0, d], az_r.at[0, d], z_peer_at(z + 1), lay)

    def down(d):
        block = wbuf.at[c, z + d, y]
        return rc(block, block, az_s.at[1, d], az_r.at[1, d], z_peer_at(z - 1), lay)

    def from_below(d):
        block = wbuf.at[c, z - d, y]
        return rc(block, block, az_s.at[0, d - 1], az_r.at[0, d - 1], z_peer_at(z - 1), lay)

    def from_above(d):
        block = wbuf.at[c, z + d, y]
        return rc(block, block, az_s.at[1, d - 1], az_r.at[1, d - 1], z_peer_at(z + 1), lay)

    def a_y(zs):
        block = wbuf.at[c, zs, y]
        return rc(block, block, ay_s.at[zs], ay_r.at[zs], y_peer, lay)

    def a_y_in(zs):
        block = wbuf.at[c, zs, yn]
        return rc(block, block, ay_s.at[zs], ay_r.at[zs], y_peer, lay)

    def a_d(cc, zs, half):
        block = wbuf.at[cc, zs, yn if half == 0 else y]
        return rc(block, block, ad_s.at[half, zs], ad_r.at[half, zs], core_peer, lay)

    to_core = rc(slab.at[0], slab.at[1], p_s.at[0], p_r.at[0], core_peer, lay)
    to_lay = rc(slab.at[0], slab.at[2], q_s.at[0], q_r.at[0], me, other)

    def has_below(d):
        return z - d >= 0

    def has_above(d):
        return z + d < R

    def when(cond):
        return pl.when(cond)

    @when(has_above(1))
    def _():
        up(0).start()

    @when(has_below(1))
    def _():
        down(0).start()

    a_y(z).start()
    to_core.start()
    a_d(c, z, 1).start()

    @pl.when(c == 1)
    def _():
        to_lay.start()

    def gather_z(d):
        @when(has_below(d))
        def _():
            from_below(d).wait_recv()

            @when(has_above(1))
            def _():
                up(d).start()

            a_y(z - d).start()
            a_d(c, z - d, 1).start()

        @when(has_above(d))
        def _():
            from_above(d).wait_recv()

            @when(has_below(1))
            def _():
                down(d).start()

            a_y(z + d).start()
            a_d(c, z + d, 1).start()

    def expand(cc, zs, yy):
        for j in range(hp):
            out[cc, zs, yy, j] = unpack(wbuf[cc, zs, yy, j])

    def sides(d, body):
        if d == 0:
            body(z)
            return

        @when(has_below(d))
        def _():
            body(z - d)

        @when(has_above(d))
        def _():
            body(z + d)

    def expand_z(d):
        sides(d, lambda zs: expand(c, zs, y))

    def gather_y(d):
        def body(zs):
            a_y_in(zs).wait_recv()
            a_d(c, zs, 0).start()
            expand(c, zs, yn)

        sides(d, body)

    def gather_core(d, half):
        def body(zs):
            a_d(1 - c, zs, half).wait_recv()
            expand(1 - c, zs, yn if half == 0 else y)

        sides(d, body)

    group = (z * 2 + y) * hp
    lane = lax.broadcasted_iota(jnp.int32, sbuf.shape[1:], 1)

    def s_out(k):
        return rc(sbuf.at[me], sbuf.at[me], ss_s.at[k], ss_r.at[k], lax.rem(me + k, n), lay)

    def s_in(k):
        src = lax.rem(me + n - k, n)
        return rc(sbuf.at[src], sbuf.at[src], ss_s.at[k], ss_r.at[k], src, lay)

    def final(k):
        @pl.when(c == k)
        def _():
            to_core.wait_recv()
            if k == 0:
                f_y().wait_recv()
            else:
                to_lay.wait_recv()
            c_y(k, R - 1).wait_recv()

            def add(slot):
                c_z_in(k, slot).wait_recv()
                for j in range(zf if k == 0 else 0, hp):
                    cp[k, z, y, j] = cp[k, z, y, j] + cz[slot, j]

            sources(z, True, add)
            for j in range(hp):
                left = slab[k, j]
                right = slab[1 + k, j]
                if k == 0 and j < zf:
                    total = cp[k, z, y, j] + cyf[j]
                else:
                    total = cp[k, z, y, j] + cy[z, j]
                zb[j] = total / token_total - dot_tt(left[D:, :], right[D:, :], HI)
            if k == 1:
                c_d(k, R - 1, 1).wait_recv()
                for j in range(hp):
                    zb[j] = zb[j] + cd[z, y, j] / token_total
            for j in range(hp):
                yb[j] = mm(slab[k, j, :D, :], zb[j])
            for j in range(hp):
                white = mm(yb[j], slab[1 + k, j, :D, :])
                zb[j] = white * white
            tile = jnp.zeros(sbuf.shape[1:], jnp.float32)
            for j in range(hp):
                value = jnp.sum(jnp.sum(zb[j], axis=0, keepdims=True), axis=1, keepdims=True) / HEAD_DIM
                tile = jnp.where(lane == group + j, value, tile)
            sbuf[me] = tile
            for q in range(1, n):
                s_out(q).start()

    for i in range(R - 1):
        cross_z(0, i, 0)
    for i in range(1, R - 1):
        first_z(i, 1)
        if i + 1 < R - 1:
            first_z(i + 1, 0)
    cross_z(1, 0, 0)
    cross_other(1, 0)
    cross_other(1, 1)
    cross_y(1, 1)
    gather_z(1)
    for d in range(2, R - 1):
        cross_other(d, 0)
        cross_y(1, d)
        gather_y(d - 2)
        gather_z(d)
        cross_other(d, 1)
        for q in range(d - 2, R - 1 if d == R - 2 else d - 1):
            cross_z(0, q, 1)
        cross_z(1, d - 2, 1)
        cross_z(1, d - 1, 0)
        expand_z(d - 1)
    gather_y(R - 3)
    gather_z(R - 1)
    cross_other(R - 1, 0)
    cross_y(1, R - 1)
    cross_z(1, R - 3, 1)
    cross_z(1, R - 2, 0)
    first_z(R - 1)
    gather_y(R - 2)
    final(0)
    expand_z(R - 2)
    expand_z(R - 1)
    cross_z(1, R - 2, 1)
    for d in range(R - 1):
        gather_core(d, 1)
    cross_other(R - 1, 1)
    final(1)
    gather_y(R - 1)
    gather_core(R - 1, 1)
    for d in range(R):
        gather_core(d, 0)

    for k in range(1, n):
        s_in(k).wait_recv()
    row0 = sbuf[0]
    row1 = sbuf[1]
    for i in range(2, n, 2):
        row0 = row0 + sbuf[i]
        row1 = row1 + sbuf[i + 1]
    sub = lax.broadcasted_iota(jnp.int32, row0.shape, 0)
    simout[...] = jnp.where(sub == lay, row0, row1)[:2, :HEADS]

    for p in range(parts):
        x_send(p).wait_send()
    for i in range(R):
        for half in range(2):
            g_d(i, half).wait_send()
            c_d(1 - c, i, half).wait_send()
        g_y(i).wait_send()
        for k in range(2):
            @pl.when(c == k)
            def _():
                c_y(k, i).wait_send()

        a_y(i).wait_send()
        for half in range(2):
            a_d(c, i, half).wait_send()
    for o in range(1, R):
        g_z(o, lowest(o)).wait_send()
    for i in range(R - 1):
        zt = ct_of(i)
        for k in range(2):
            @pl.when(c == k)
            def _():
                c_z(k, zt, slot_of(zt)).wait_send()
                if k == 0:
                    f_z(zt, slot_of(zt)).wait_send()

    for d in range(R - 1):
        @when(jnp.logical_and(has_below(d), has_above(1)))
        def _():
            up(d).wait_send()

        @when(jnp.logical_and(has_above(d), has_below(1)))
        def _():
            down(d).wait_send()

    to_core.wait_send()

    @pl.when(c == 0)
    def _():
        f_y().wait_send()

    @pl.when(c == 1)
    def _():
        to_lay.wait_send()

    for k in range(1, n):
        s_out(k).wait_send()


def solution(mesh):
    n = mesh.shape["tok"]
    R = n // 4
    hp = -(-HEADS // (n // 2))
    zf = max(hp * Z_FIRST // 5, 1)
    D = HEAD_DIM
    E = hp * PACKED + PAD
    parts = 1 if R * 2 * hp != HEADS else 2 * R

    def local(first_acts, second_acts):
        _, rows, width = first_acts.shape
        token_total = float(rows * n)
        f32 = jnp.float32
        bf16 = jnp.bfloat16
        dma = lambda *k: pltpu.SemaphoreType.DMA(tuple(max(q, 1) for q in k))
        out, sims = pl.pallas_call(
            functools.partial(kernel, n, R, hp, zf, token_total),
            out_shape=(
                pltpu.VMEM((2, R, 2, hp, D, D), f32),
                pltpu.VMEM((2, HEADS), f32),
            ),
            in_specs=[pl.BlockSpec(memory_space=pltpu.MemorySpace.HBM)] * 2,
            out_specs=(
                pl.BlockSpec(memory_space=pltpu.VMEM),
                pl.BlockSpec(memory_space=pltpu.VMEM),
            ),
            scratch_shapes=[
                pltpu.VMEM((rows, width), bf16),
                pltpu.VMEM((rows, width), bf16),
                pltpu.VMEM((rows, width), bf16),
                pltpu.VMEM((2, R, 2, E, D), f32),
                pltpu.VMEM((R, 2, E, D), f32),
                pltpu.VMEM((R, E, D), f32),
                pltpu.VMEM((R - 1, E, D), f32),
                pltpu.VMEM((2, R, 2, hp, D, D), f32),
                pltpu.VMEM((R, 2, hp, D, D), f32),
                pltpu.VMEM((R, hp, D, D), f32),
                pltpu.VMEM((R + 1, hp, D, D), f32),
                pltpu.VMEM((zf, D, D), f32),
                pltpu.VMEM((R + 1, 2, zf, D, D), f32),
                pltpu.VMEM((3, hp, D + PAD, D), f32),
                pltpu.VMEM((2, R, 2, hp, PACKED, D), f32),
                pltpu.VMEM((n, 8, D), f32),
                pltpu.VMEM((hp, D, D), f32),
                pltpu.VMEM((hp, D, D), f32),
                dma(2 * parts), dma(parts), dma(parts),
                dma(2, R), dma(2, R), dma(R), dma(R), dma(R - 1), dma(R - 1),
                dma(2, R), dma(2, R), dma(R), dma(R), dma(R + 1), dma(R + 1), dma(1), dma(1), dma(R + 1), dma(R + 1),
                dma(1), dma(1), dma(1), dma(1),
                dma(2, R), dma(2, R), dma(R), dma(R), dma(2, R), dma(2, R),
                dma(n), dma(n),
            ],
            compiler_params=pltpu.CompilerParams(
                collective_id=0, has_side_effects=True, vmem_limit_bytes=VMEM_LIMIT
            ),
        )(first_acts[0], second_acts[0])
        whitening = out.reshape(2, R * 2 * hp, D, D)[:, None, :HEADS]
        return whitening, sims[None]

    in_specs = (P("lay", "tok", None), P("lay", "tok", None))
    out_specs = (P(None, "lay", None, None, None), P("lay", None, None))
    return jax.shard_map(local, mesh=mesh, in_specs=in_specs, out_specs=out_specs, check_vma=False)
```

```python
import functools

import jax
import jax.numpy as jnp
from jax import lax
from jax.experimental import pallas as pl
from jax.experimental.pallas import tpu as pltpu
from jax.sharding import PartitionSpec as P

HEADS = 40
HEAD_DIM = 128
ITERS = 6
PAD = 8

ridge_weight = 0.05
Z_FIRST = 2
VMEM_LIMIT = 54 * 1024 * 1024
MESH = pl.DeviceIdType.MESH
HI = lax.Precision.HIGHEST


def dot_tt(a, b, precision=None):
    return lax.dot_general(
        a, b, (((0,), (0,)), ((), ())), preferred_element_type=jnp.float32, precision=precision
    )


def mm(a, b):
    return jnp.dot(a, b, preferred_element_type=jnp.float32, precision=HI)


BLOCKS = HEAD_DIM // 8
KEPT = BLOCKS // 2 + 1
PACKED = 8 * KEPT


def lane_block():
    return lax.broadcasted_iota(jnp.int32, (8, HEAD_DIM), 1) // 8


def pack(a):
    lb = lane_block()
    xs = [a[8 * e : 8 * e + 8, :] for e in range(BLOCKS)]
    step = 1
    while step < BLOCKS:
        bit = (lb // step) % 2 == 1
        xs = [jnp.where(bit, xs[(e + step) % BLOCKS], xs[e]) for e in range(BLOCKS)]
        step *= 2
    return jnp.concatenate([xs[(-d) % BLOCKS] for d in range(KEPT)], axis=0)


def unpack(p):
    lb = lane_block()
    zero = jnp.zeros((8, HEAD_DIM), jnp.float32)
    ys = [zero] * BLOCKS
    for d in range(KEPT):
        ys[(-d) % BLOCKS] = p[8 * d : 8 * d + 8, :]
    step = 1
    while step < BLOCKS:
        bit = (lb // step) % 2 == 1
        ys = [jnp.where(bit, ys[(e - step) % BLOCKS], ys[e]) for e in range(BLOCKS)]
        step *= 2
    half = jnp.concatenate(ys, axis=0)
    rb = lax.broadcasted_iota(jnp.int32, (HEAD_DIM, HEAD_DIM), 0) // 8
    cb = lax.broadcasted_iota(jnp.int32, (HEAD_DIM, HEAD_DIM), 1) // 8
    return jnp.where((cb - rb + BLOCKS) % BLOCKS < KEPT, half, half.T)


def kernel(
    n, R, hp, zf, token_total,
    x1h, x2h, out, simout,
    x1, x2, x2o, gp, gd, gy, gz, cp, cd, cy, cz, cyf, czf, slab, wlay, wbuf, sbuf, yb, zb,
    l_s, x_s, x_r, gd_s, gd_r, gy_s, gy_r, gz_s, gz_r,
    cd_s, cd_r, cy_s, cy_r, cz_s, cz_r, fy_s, fy_r, fz_s, fz_r,
    p_s, p_r, q_s, q_r, az_s, az_r, ay_s, ay_r, ad_s, ad_r, ss_s, ss_r,
):
    me = lax.axis_index("tok")
    lay = lax.axis_index("lay")
    other = 1 - lay
    c = lax.rem(me, 2)
    y = lax.rem(me // 2, 2)
    z = me // 4
    yn = 1 - y
    rows = x1.shape[0]
    D = HEAD_DIM
    core_peer = z * 4 + y * 2 + (1 - c)
    y_peer = z * 4 + yn * 2 + c
    padded = R * 2 * hp != HEADS

    bits = [1 << t for t in range(R.bit_length() - 1)]

    def z_xor(o):
        total = 0
        for b in bits:
            zb = lax.rem(z // b, 2)
            ob = lax.rem(o // b, 2) if not isinstance(o, int) else o // b % 2
            total = total + b * (zb + ob - 2 * zb * ob)
        return total

    def z_peer_at(zt):
        return zt * 4 + y * 2 + c

    def z_peer(o):
        return z_xor(o) * 4 + y * 2 + c

    def at_least(a, b):
        return (a - b + R) // R

    def ct_of(i):
        step = R - 1 - i
        below = z
        above = R - 1 - z
        short = jnp.minimum(below, above)
        up_far = at_least(above, below)
        paired = 1 - at_least(step, 2 * short + 1)
        dist = paired * ((step + 1) // 2) + (1 - paired) * (step - short)
        near_side = paired * (1 - lax.rem(step, 2))
        up = up_far + near_side - 2 * up_far * near_side
        return z + dist * (2 * up - 1)

    def hop(zt):
        return 2 * at_least(zt, z) - 1

    def slot_of(zt):
        direction = hop(zt)
        last = (R - direction * (zt - z)) // (R - 1)
        down = (1 - direction) // 2
        return zt + (R - zt) * last * down

    def has_source(zt):
        return inside(z - hop(zt))

    def inside(q):
        return at_least(q, 0) * at_least(R - 1, q)

    def terms_of(o):
        return [b for b in bits if o % (2 * b) == 0]

    def lowest(o):
        return next(b for b in bits if o // b % 2)

    def rc(src, dst, s, r, tok, ly):
        return pltpu.make_async_remote_copy(
            src_ref=src, dst_ref=dst, send_sem=s, recv_sem=r,
            device_id=(tok, ly), device_id_type=MESH,
        )

    def zt_of(i):
        return z_xor(R - 1 - i)

    barrier = pltpu.get_barrier_semaphore()
    for k in range(1, n):
        pl.semaphore_signal(barrier, inc=1, device_id=(lax.rem(me + k, n), lay), device_id_type=MESH)
    pl.semaphore_signal(barrier, inc=1, device_id=(me, other), device_id_type=MESH)

    parts = 1 if padded else 2 * R
    width = x1.shape[1] // parts

    def part_cols(p):
        if padded:
            return pl.ds(0, width)
        half = yn if p % 2 == 0 else y
        return pl.ds(pl.multiple_of((ct_of(p // 2) * 2 + half) * width, 128), width)

    load_x2 = pltpu.make_async_copy(x2h, x2, l_s.at[0])
    load_x1 = pltpu.make_async_copy(x1h, x1, l_s.at[1])
    load_x2.start()
    load_x1.start()

    def x_send(p):
        cols = part_cols(p)
        return rc(x2.at[:, cols], x2o.at[:, cols], x_s.at[0], x_r.at[p], me, other)

    pl.semaphore_wait(barrier, n)
    load_x2.wait()
    for p in range(parts):
        x_send(p).start()
    load_x1.wait()

    def head_cols(zt, yy, j):
        h = (zt * 2 + yy) * hp + j
        if padded:
            h = jnp.minimum(h, HEADS - 1)
        return pl.ds(pl.multiple_of(h * D, D), D)

    ones = jnp.ones((PAD, rows), jnp.bfloat16)
    sub8 = lax.broadcasted_iota(jnp.int32, (PAD, D), 0)

    def gram_half(i, half):
        zt = zt_of(i)
        yy = yn if half == 0 else y
        sums = [jnp.zeros((PAD, D), jnp.float32)] * 2
        for j in range(hp):
            cols = head_cols(zt, yy, j)
            for k, ref in enumerate((x1, x2)):
                v = ref[:, cols]
                gp[k, zt, yy, j * PACKED : (j + 1) * PACKED, :] = pack(dot_tt(v, v))
                sums[k] = jnp.where(sub8 == j, jnp.dot(ones, v, preferred_element_type=jnp.float32), sums[k])
        for k in range(2):
            gp[k, zt, yy, hp * PACKED :, :] = sums[k]
        g_d(i, half).start()

    def g_d(i, half):
        zt = zt_of(i)
        yy = yn if half == 0 else y
        return rc(gp.at[1 - c, zt, yy], gd.at[zt, yy], gd_s.at[0], gd_r.at[half, i], core_peer, lay)

    def g_y(i):
        zt = zt_of(i)
        return rc(gp.at[c, zt, yn], gy.at[zt], gy_s.at[0], gy_r.at[i], y_peer, lay)

    def g_z(o, b):
        return rc(gp.at[c, z_xor(o), y], gz.at[o - 1], gz_s.at[0], gz_r.at[o - 1], z_peer(b), lay)

    def g_yph(i):
        zt = zt_of(i)
        g_d(i, 0).wait_recv()
        gp[c, zt, yn] = gp[c, zt, yn] + gd[zt, yn]
        g_y(i).start()

    def g_zph(i):
        zt = zt_of(i)
        o = R - 1 - i
        g_d(i, 1).wait_recv()
        g_y(i).wait_recv()
        terms = terms_of(o) if o else []
        for b in terms:
            g_z(o + b, b).wait_recv()
        total = gp[c, zt, y] + gd[zt, y] + gy[zt]
        for b in terms:
            total = total + gz[o + b - 1]
        gp[c, zt, y] = total
        if o:
            g_z(o, lowest(o)).start()

    def first_body(i, carry):
        gram_half(i, 0)

        @pl.when(i >= 1)
        def _():
            g_yph(i - 1)

        return carry

    def second_body(i, carry):
        gram_half(i, 1)

        @pl.when(i == 0)
        def _():
            g_yph(R - 1)

        return carry

    lax.fori_loop(0, R, first_body, 0)

    def c_d(k, i, half):
        zt = ct_of(i)
        yy = yn if half == 0 else y
        return rc(cp.at[k, zt, yy], cd.at[zt, yy], cd_s.at[0], cd_r.at[half, i], core_peer, lay)

    def own_heads(k):
        return pl.ds(zf, hp - zf) if k == 0 else pl.ds(0, hp)

    def c_y(k, i):
        zt = ct_of(i)
        hs = own_heads(k)
        return rc(cp.at[k, zt, yn, hs], cy.at[zt, hs], cy_s.at[0], cy_r.at[i], y_peer, lay)

    def c_z(k, zt, slot):
        hs = own_heads(k)
        return rc(cp.at[k, zt, y, hs], cz.at[slot, hs], cz_s.at[0], cz_r.at[slot], z_peer_at(z + hop(zt)), lay)

    def c_z_in(k, slot):
        hs = own_heads(k)
        return rc(cp.at[k, z, y, hs], cz.at[slot, hs], cz_s.at[0], cz_r.at[slot], me, other)

    def f_z(zt, slot):
        return rc(
            cp.at[0, zt, :, pl.ds(0, zf)], czf.at[slot], fz_s.at[0], fz_r.at[slot], z_peer_at(z + hop(zt)), lay
        )

    def f_z_in(slot):
        return rc(cp.at[0, z, :, pl.ds(0, zf)], czf.at[slot], fz_s.at[0], fz_r.at[slot], me, other)

    def f_y():
        return rc(cp.at[0, z, yn, pl.ds(0, zf)], cyf, fy_s.at[0], fy_r.at[0], y_peer, lay)

    def sources(zt, own, body):
        if own:
            pl.when(z > 0)(lambda: body(z))
            pl.when(z < R - 1)(lambda: body(R))
        else:
            pl.when(has_source(zt) == 1)(lambda: body(zt))

    def first_z(i, chained=None):
        ready = c == 1
        if chained is not None:
            ready = jnp.logical_and(ready, has_source(ct_of(i)) == chained)

        @pl.when(ready)
        def _():
            own = i == R - 1
            zt = ct_of(i)

            def add(slot):
                f_z_in(slot).wait_recv()
                for half in range(2):
                    for j in range(zf):
                        cp[0, zt, half, j] = cp[0, zt, half, j] + czf[slot, half, j]

            sources(zt, own, add)
            if own:
                f_y().start()
            else:
                f_z(zt, slot_of(zt)).start()

    def cross_half(k, i, half):
        zt = ct_of(i)
        yy = yn if half == 0 else y
        ref = x2 if k == 0 else x2o
        for j in range(hp):
            cols = head_cols(zt, yy, j)
            cp[k, zt, yy, j] = dot_tt(x1[:, cols], ref[:, cols])

        @pl.when(c == k)
        def _():
            c_d(k, i, half).start()

    def cross_y(k, i):
        @pl.when(c == 1 - k)
        def _():
            zt = ct_of(i)
            c_d(k, i, 0).wait_recv()
            for j in range(hp):
                cp[k, zt, yn, j] = cp[k, zt, yn, j] + cd[zt, yn, j]
            c_y(k, i).start()
            if k == 0:
                c_d(k, i, 1).wait_recv()
                for j in range(hp):
                    cp[k, zt, y, j] = cp[k, zt, y, j] + cd[zt, y, j]

    def cross_z(k, i, chained):
        @pl.when(jnp.logical_and(c == 1 - k, has_source(ct_of(i)) == chained))
        def _():
            zt = ct_of(i)
            if k == 1:
                c_d(k, i, 1).wait_recv()
            c_y(k, i).wait_recv()
            for j in range(zf if k == 0 else 0, hp):
                total = cp[k, zt, y, j] + cy[zt, j]
                if k == 1:
                    total = total + cd[zt, y, j]
                cp[k, zt, y, j] = total

            def add(slot):
                c_z_in(k, slot).wait_recv()
                for j in range(zf if k == 0 else 0, hp):
                    cp[k, zt, y, j] = cp[k, zt, y, j] + cz[slot, j]

            sources(zt, False, add)
            c_z(k, zt, slot_of(zt)).start()

    def loop(body, lo, hi):
        def step(i, carry):
            body(i)
            return carry

        lax.fori_loop(lo, hi, step, 0)

    def cross_own(i):
        cross_half(0, i, 0)
        cross_half(0, i, 1)

    def cross_other(i, half):
        p = 2 * i + half
        if p < parts:
            x_send(p).wait_recv()
        cross_half(1, i, half)

    cross_own(0)
    lax.fori_loop(0, R, second_body, 0)
    cross_y(0, 0)
    first_z(0, 0)
    loop(cross_own, 1, R)
    g_zph(0)
    loop(lambda i: cross_y(0, i), 1, R)
    for i in range(1, R - 1):
        g_zph(i)
        if i == 1:
            first_z(0, 1)
            first_z(1, 0)
    cross_other(0, 0)
    cross_other(0, 1)
    g_zph(R - 1)
    cross_y(1, 0)
    for b in bits:
        g_z(b, b).wait_recv()

    eye = (
        lax.broadcasted_iota(jnp.int32, (D, D), 0) == lax.broadcasted_iota(jnp.int32, (D, D), 1)
    ).astype(jnp.float32)
    scales = []
    tail = slice(hp * PACKED, hp * PACKED + PAD)
    col_sums = gp[c, z, y, tail, :]
    for b in bits:
        col_sums = col_sums + gz[b - 1, tail, :]
    for j in range(hp):
        at = slice(j * PACKED, (j + 1) * PACKED)
        total = gp[c, z, y, at, :]
        for b in bits:
            total = total + gz[b - 1, at, :]
        mean = jnp.where(sub8 == 0, col_sums[j : j + 1, :], 0.0) / token_total
        slab[0, j, D:, :] = mean
        cov = unpack(total) / token_total - dot_tt(mean, mean, HI) + ridge_weight * eye
        norm2 = jnp.sum(jnp.sum(cov * cov, axis=1, keepdims=True), axis=0, keepdims=True)
        scale = jnp.sqrt(norm2)
        scales.append(scale)
        y0 = cov / scale
        f = 1.5 * eye - 0.5 * y0
        yb[j] = mm(y0, f)
        zb[j] = f

    def ns_body(t, carry):
        fs = [1.5 * eye - 0.5 * mm(zb[j], yb[j]) for j in range(hp)]
        for j in range(hp):
            yb[j] = mm(yb[j], fs[j])
            zb[j] = mm(fs[j], zb[j])
        return carry

    lax.fori_loop(1, ITERS - 1, ns_body, 0)
    for j in range(hp):
        f = 1.5 * eye - 0.5 * mm(zb[j], yb[j])
        w = mm(f, zb[j]) / jnp.sqrt(scales[j])
        slab[0, j, :D, :] = w
        wbuf[c, z, y, j] = pack(w)
        out[c, z, y, j] = w

    def up(d):
        block = wbuf.at[c, z - d, y]
        return rc(block, block, az_s.at[0, d], az_r.at[0, d], z_peer_at(z + 1), lay)

    def down(d):
        block = wbuf.at[c, z + d, y]
        return rc(block, block, az_s.at[1, d], az_r.at[1, d], z_peer_at(z - 1), lay)

    def from_below(d):
        block = wbuf.at[c, z - d, y]
        return rc(block, block, az_s.at[0, d - 1], az_r.at[0, d - 1], z_peer_at(z - 1), lay)

    def from_above(d):
        block = wbuf.at[c, z + d, y]
        return rc(block, block, az_s.at[1, d - 1], az_r.at[1, d - 1], z_peer_at(z + 1), lay)

    def a_y(zs):
        block = wbuf.at[c, zs, y]
        return rc(block, block, ay_s.at[0], ay_r.at[zs], y_peer, lay)

    def a_y_in(zs):
        block = wbuf.at[c, zs, yn]
        return rc(block, block, ay_s.at[0], ay_r.at[zs], y_peer, lay)

    def a_d(cc, zs, half):
        block = wbuf.at[cc, zs, yn if half == 0 else y]
        return rc(block, block, ad_s.at[0], ad_r.at[half, zs], core_peer, lay)

    to_core = rc(slab.at[0], slab.at[1], p_s.at[0], p_r.at[0], core_peer, lay)
    to_lay = [
        rc(wbuf.at[1, z, y], wlay, q_s.at[0], q_r.at[0], core_peer, other),
        rc(slab.at[0, :, pl.ds(D, PAD)], slab.at[2, :, pl.ds(D, PAD)], q_s.at[1], q_r.at[1], core_peer, other),
    ]

    def has_below(d):
        return z - d >= 0

    def has_above(d):
        return z + d < R

    def when(cond):
        return pl.when(cond)

    @when(has_above(1))
    def _():
        up(0).start()

    @when(has_below(1))
    def _():
        down(0).start()

    a_y(z).start()
    to_core.start()
    a_d(c, z, 1).start()

    @pl.when(c == 1)
    def _():
        to_lay[1].start()
        to_lay[0].start()

    def gather_z(d):
        @when(has_below(d))
        def _():
            from_below(d).wait_recv()

            @when(has_above(1))
            def _():
                up(d).start()

            a_y(z - d).start()
            a_d(c, z - d, 1).start()

        @when(has_above(d))
        def _():
            from_above(d).wait_recv()

            @when(has_below(1))
            def _():
                down(d).start()

            a_y(z + d).start()
            a_d(c, z + d, 1).start()

    def expand(cc, zs, yy):
        for j in range(hp):
            out[cc, zs, yy, j] = unpack(wbuf[cc, zs, yy, j])

    def sides(d, body):
        if d == 0:
            body(z)
            return

        @when(has_below(d))
        def _():
            body(z - d)

        @when(has_above(d))
        def _():
            body(z + d)

    def expand_z(d):
        sides(d, lambda zs: expand(c, zs, y))

    def gather_y(d):
        def body(zs):
            a_y_in(zs).wait_recv()
            a_d(c, zs, 0).start()
            expand(c, zs, yn)

        sides(d, body)

    def gather_core(d, half):
        def body(zs):
            a_d(1 - c, zs, half).wait_recv()
            expand(1 - c, zs, yn if half == 0 else y)

        sides(d, body)

    group = (z * 2 + y) * hp
    lane = lax.broadcasted_iota(jnp.int32, sbuf.shape[1:], 1)

    def s_out(k):
        return rc(sbuf.at[me], sbuf.at[me], ss_s.at[0], ss_r.at[0], lax.rem(me + k, n), lay)

    def final(k):
        left_at, right_at = (1, 0) if k == 0 else (0, 2)

        @pl.when(c == 1 - k)
        def _():
            to_core.wait_recv()
            if k == 0:
                f_y().wait_recv()
            else:
                for d in to_lay[::-1]:
                    d.wait_recv()
                for j in range(hp):
                    slab[2, j, :D, :] = unpack(wlay[j])
            c_y(k, R - 1).wait_recv()

            def add(slot):
                c_z_in(k, slot).wait_recv()
                for j in range(zf if k == 0 else 0, hp):
                    cp[k, z, y, j] = cp[k, z, y, j] + cz[slot, j]

            sources(z, True, add)
            for j in range(hp):
                left = slab[left_at, j]
                right = slab[right_at, j]
                if k == 0 and j < zf:
                    total = cp[k, z, y, j] + cyf[j]
                else:
                    total = cp[k, z, y, j] + cy[z, j]
                zb[j] = total / token_total - dot_tt(left[D:, :], right[D:, :], HI)
            if k == 1:
                c_d(k, R - 1, 1).wait_recv()
                for j in range(hp):
                    zb[j] = zb[j] + cd[z, y, j] / token_total
            for j in range(hp):
                yb[j] = mm(slab[left_at, j, :D, :], zb[j])
            for j in range(hp):
                white = mm(yb[j], slab[right_at, j, :D, :])
                zb[j] = white * white
            tile = jnp.zeros(sbuf.shape[1:], jnp.float32)
            for j in range(hp):
                value = jnp.sum(jnp.sum(zb[j], axis=0, keepdims=True), axis=1, keepdims=True) / HEAD_DIM
                tile = jnp.where(lane == group + j, value, tile)
            sbuf[me] = tile
            for q in range(1, n):
                s_out(q).start()

    for i in range(R - 1):
        cross_z(0, i, 0)
    for i in range(1, R - 1):
        first_z(i, 1)
        if i + 1 < R - 1:
            first_z(i + 1, 0)
    cross_z(1, 0, 0)
    cross_other(1, 0)
    cross_other(1, 1)
    cross_y(1, 1)
    gather_z(1)
    for d in range(2, R - 1):
        cross_other(d, 0)
        cross_y(1, d)
        gather_y(d - 2)
        gather_z(d)
        cross_other(d, 1)
        for q in range(d - 2, R - 1 if d == R - 2 else d - 1):
            cross_z(0, q, 1)
        cross_z(1, d - 2, 1)
        cross_z(1, d - 1, 0)
        expand_z(d - 1)
    gather_z(R - 1)
    cross_z(1, R - 2, 0)
    gather_y(R - 3)
    cross_other(R - 1, 0)
    cross_y(1, R - 1)
    cross_z(1, R - 3, 1)
    cross_z(1, R - 2, 1)
    first_z(R - 1)
    gather_y(R - 2)
    expand_z(R - 2)
    expand_z(R - 1)
    for d in range(R - 1):
        gather_core(d, 1)
    cross_other(R - 1, 1)
    final(0)
    final(1)
    gather_y(R - 1)
    gather_core(R - 1, 1)
    for d in range(R):
        gather_core(d, 0)

    def sent(ref, sem):
        rc(ref, ref, sem.at[0], sem.at[0], core_peer, lay).wait_send()

    sent(x2, x_s)
    sent(gd, gd_s)
    sent(gy, gy_s)
    sent(gz, gz_s)
    sent(cd, cd_s)
    sent(wbuf.at[c, :, y], ay_s)
    sent(wbuf.at[c], ad_s)
    for k in range(2):
        @pl.when(c == 1 - k)
        def _():
            hs = own_heads(k)
            sent(cy.at[:, hs], cy_s)
            sent(cz.at[pl.ds(0, R - 1), hs], cz_s)
            if k == 0:
                sent(czf.at[pl.ds(0, R - 1)], fz_s)
                f_y().wait_send()

    for d in range(R - 1):
        @when(jnp.logical_and(has_below(d), has_above(1)))
        def _():
            up(d).wait_send()

        @when(jnp.logical_and(has_above(d), has_below(1)))
        def _():
            down(d).wait_send()

    to_core.wait_send()

    @pl.when(c == 1)
    def _():
        for d in to_lay:
            d.wait_send()

    tiles = sbuf.at[pl.ds(0, n - 1)]
    sent(tiles, ss_s)
    rc(tiles, tiles, ss_s.at[0], ss_r.at[0], core_peer, lay).wait_recv()
    row0 = sbuf[0]
    row1 = sbuf[1]
    for i in range(2, n, 2):
        row0 = row0 + sbuf[i]
        row1 = row1 + sbuf[i + 1]
    sub = lax.broadcasted_iota(jnp.int32, row0.shape, 0)
    simout[...] = jnp.where(sub == lay, row1, row0)[:2, :HEADS]


def solution(mesh):
    n = mesh.shape["tok"]
    R = n // 4
    hp = -(-HEADS // (n // 2))
    zf = max(hp * Z_FIRST // 5, 1)
    D = HEAD_DIM
    E = hp * PACKED + PAD
    parts = 1 if R * 2 * hp != HEADS else 2 * R

    def local(first_acts, second_acts):
        _, rows, width = first_acts.shape
        token_total = float(rows * n)
        f32 = jnp.float32
        bf16 = jnp.bfloat16
        dma = lambda *k: pltpu.SemaphoreType.DMA(tuple(max(q, 1) for q in k))
        out, sims = pl.pallas_call(
            functools.partial(kernel, n, R, hp, zf, token_total),
            out_shape=(
                pltpu.VMEM((2, R, 2, hp, D, D), f32),
                pltpu.VMEM((2, HEADS), f32),
            ),
            in_specs=[pl.BlockSpec(memory_space=pltpu.MemorySpace.HBM)] * 2,
            out_specs=(
                pl.BlockSpec(memory_space=pltpu.VMEM),
                pl.BlockSpec(memory_space=pltpu.VMEM),
            ),
            scratch_shapes=[
                pltpu.VMEM((rows, width), bf16),
                pltpu.VMEM((rows, width), bf16),
                pltpu.VMEM((rows, width), bf16),
                pltpu.VMEM((2, R, 2, E, D), f32),
                pltpu.VMEM((R, 2, E, D), f32),
                pltpu.VMEM((R, E, D), f32),
                pltpu.VMEM((R - 1, E, D), f32),
                pltpu.VMEM((2, R, 2, hp, D, D), f32),
                pltpu.VMEM((R, 2, hp, D, D), f32),
                pltpu.VMEM((R, hp, D, D), f32),
                pltpu.VMEM((R + 1, hp, D, D), f32),
                pltpu.VMEM((zf, D, D), f32),
                pltpu.VMEM((R + 1, 2, zf, D, D), f32),
                pltpu.VMEM((3, hp, D + PAD, D), f32),
                pltpu.VMEM((hp, PACKED, D), f32),
                pltpu.VMEM((2, R, 2, hp, PACKED, D), f32),
                pltpu.VMEM((n, 8, D), f32),
                pltpu.VMEM((hp, D, D), f32),
                pltpu.VMEM((hp, D, D), f32),
                dma(2), dma(1), dma(parts),
                dma(1), dma(2, R), dma(1), dma(R), dma(1), dma(R - 1),
                dma(1), dma(2, R), dma(1), dma(R), dma(1), dma(R + 1),
                dma(1), dma(1), dma(1), dma(R + 1),
                dma(1), dma(1), dma(2), dma(2),
                dma(2, R - 1), dma(2, R - 1), dma(1), dma(R), dma(1), dma(2, R),
                dma(1), dma(1),
            ],
            compiler_params=pltpu.CompilerParams(
                collective_id=0, has_side_effects=True, vmem_limit_bytes=VMEM_LIMIT
            ),
        )(first_acts[0], second_acts[0])
        whitening = out.reshape(2, R * 2 * hp, D, D)[:, None, :HEADS]
        return whitening, sims[None]

    in_specs = (P("lay", "tok", None), P("lay", "tok", None))
    out_specs = (P(None, "lay", None, None, None), P("lay", None, None))
    return jax.shard_map(local, mesh=mesh, in_specs=in_specs, out_specs=out_specs, check_vma=False)
```

```python
import functools

import jax
import jax.numpy as jnp
from jax import lax
from jax.experimental import pallas as pl
from jax.experimental.pallas import tpu as pltpu
from jax.sharding import PartitionSpec as P

HEADS = 40
HEAD_DIM = 128
ITERS = 6
PAD = 8

ridge_weight = 0.05
Z_FIRST = 2
VMEM_LIMIT = 54 * 1024 * 1024
MESH = pl.DeviceIdType.MESH
HI = lax.Precision.HIGHEST


def dot_tt(a, b, precision=None):
    return lax.dot_general(
        a, b, (((0,), (0,)), ((), ())), preferred_element_type=jnp.float32, precision=precision
    )


def mm(a, b):
    return jnp.dot(a, b, preferred_element_type=jnp.float32, precision=HI)


BLOCKS = HEAD_DIM // 8
KEPT = BLOCKS // 2 + 1
MAIN = 8 * (KEPT - 1)


def lane_block():
    return lax.broadcasted_iota(jnp.int32, (8, HEAD_DIM), 1) // 8


def pack(a):
    lb = lane_block()
    xs = [a[8 * e : 8 * e + 8, :] for e in range(BLOCKS)]
    step = 1
    while step < BLOCKS:
        bit = (lb // step) % 2 == 1
        xs = [jnp.where(bit, xs[(e + step) % BLOCKS], xs[e]) for e in range(BLOCKS)]
        step *= 2
    return jnp.concatenate([xs[(-d) % BLOCKS] for d in range(KEPT)], axis=0)


def packed_rows(hp):
    return hp * MAIN + (hp + 1) // 2 * 8


def store_packed(ref, blocks):
    hp = len(blocks)
    first = lax.broadcasted_iota(jnp.int32, (8, HEAD_DIM), 1) < HEAD_DIM // 2
    for j in range(hp):
        ref[j * MAIN : (j + 1) * MAIN, :] = blocks[j][:MAIN, :]
    for t in range((hp + 1) // 2):
        left, right = blocks[2 * t], blocks[min(2 * t + 1, hp - 1)]
        ref[hp * MAIN + 8 * t : hp * MAIN + 8 * t + 8, :] = jnp.where(first, left[MAIN:, :], right[MAIN:, :])


def load_packed(read, hp, j):
    at = hp * MAIN + 8 * (j // 2)
    return unpack(jnp.concatenate([read(j * MAIN, (j + 1) * MAIN), read(at, at + 8)], axis=0), j % 2)


def unpack(p, odd):
    lb = lane_block()
    zero = jnp.zeros((8, HEAD_DIM), jnp.float32)
    ys = [zero] * BLOCKS
    for d in range(KEPT):
        ys[(-d) % BLOCKS] = p[8 * d : 8 * d + 8, :]
    step = 1
    while step < BLOCKS:
        bit = (lb // step) % 2 == 1
        ys = [jnp.where(bit, ys[(e - step) % BLOCKS], ys[e]) for e in range(BLOCKS)]
        step *= 2
    half = jnp.concatenate(ys, axis=0)
    rb = lax.broadcasted_iota(jnp.int32, (HEAD_DIM, HEAD_DIM), 0) // 8
    cb = lax.broadcasted_iota(jnp.int32, (HEAD_DIM, HEAD_DIM), 1) // 8
    away = (cb - rb + BLOCKS) % BLOCKS
    side = cb >= BLOCKS // 2 if odd else cb < BLOCKS // 2
    keep = jnp.logical_or(away < KEPT - 1, jnp.logical_and(away == KEPT - 1, side))
    return jnp.where(keep, half, half.T)


def kernel(
    n, R, hp, zf, token_total,
    x1h, x2h, out, simout,
    x1, x2, x2o, gp, gd, gy, gz, cp, cd, cy, cz, cyf, czf, slab, wlay, wbuf, sbuf, yb, zb,
    l_s, x_s, x_r, gd_s, gd_r, gy_s, gy_r, gz_s, gz_r,
    cd_s, cd_r, cy_s, cy_r, cz_s, cz_r, fy_s, fy_r, fz_s, fz_r,
    p_s, p_r, q_s, q_r, az_s, az_r, ay_s, ay_r, ad_s, ad_r, ss_s, ss_r,
):
    me = lax.axis_index("tok")
    lay = lax.axis_index("lay")
    other = 1 - lay
    c = lax.rem(me, 2)
    y = lax.rem(me // 2, 2)
    z = me // 4
    yn = 1 - y
    rows = x1.shape[0]
    D = HEAD_DIM
    core_peer = z * 4 + y * 2 + (1 - c)
    y_peer = z * 4 + yn * 2 + c
    padded = R * 2 * hp != HEADS

    bits = [1 << t for t in range(R.bit_length() - 1)]

    def z_xor(o):
        total = 0
        for b in bits:
            zb = lax.rem(z // b, 2)
            ob = lax.rem(o // b, 2) if not isinstance(o, int) else o // b % 2
            total = total + b * (zb + ob - 2 * zb * ob)
        return total

    def z_peer_at(zt):
        return zt * 4 + y * 2 + c

    def z_peer(o):
        return z_xor(o) * 4 + y * 2 + c

    def at_least(a, b):
        return (a - b + R) // R

    def ct_of(i):
        step = R - 1 - i
        below = z
        above = R - 1 - z
        short = jnp.minimum(below, above)
        up_far = at_least(above, below)
        paired = 1 - at_least(step, 2 * short + 1)
        dist = paired * ((step + 1) // 2) + (1 - paired) * (step - short)
        near_side = paired * (1 - lax.rem(step, 2))
        up = up_far + near_side - 2 * up_far * near_side
        return z + dist * (2 * up - 1)

    def hop(zt):
        return 2 * at_least(zt, z) - 1

    def slot_of(zt):
        direction = hop(zt)
        last = (R - direction * (zt - z)) // (R - 1)
        down = (1 - direction) // 2
        return zt + (R - zt) * last * down

    def has_source(zt):
        return inside(z - hop(zt))

    def inside(q):
        return at_least(q, 0) * at_least(R - 1, q)

    def terms_of(o):
        return [b for b in bits if o % (2 * b) == 0]

    def lowest(o):
        return next(b for b in bits if o // b % 2)

    def rc(src, dst, s, r, tok, ly):
        return pltpu.make_async_remote_copy(
            src_ref=src, dst_ref=dst, send_sem=s, recv_sem=r,
            device_id=(tok, ly), device_id_type=MESH,
        )

    def zt_of(i):
        return z_xor(R - 1 - i)

    barrier = pltpu.get_barrier_semaphore()
    for k in range(1, n):
        pl.semaphore_signal(barrier, inc=1, device_id=(lax.rem(me + k, n), lay), device_id_type=MESH)
    pl.semaphore_signal(barrier, inc=1, device_id=(me, other), device_id_type=MESH)

    parts = 1 if padded else 2 * R
    width = x1.shape[1] // parts

    def part_cols(p):
        if padded:
            return pl.ds(0, width)
        half = yn if p % 2 == 0 else y
        return pl.ds(pl.multiple_of((ct_of(p // 2) * 2 + half) * width, 128), width)

    load_x2 = pltpu.make_async_copy(x2h, x2, l_s.at[0])
    load_x1 = pltpu.make_async_copy(x1h, x1, l_s.at[1])
    load_x2.start()
    load_x1.start()

    def x_send(p):
        cols = part_cols(p)
        return rc(x2.at[:, cols], x2o.at[:, cols], x_s.at[0], x_r.at[p], me, other)

    pl.semaphore_wait(barrier, n)
    load_x2.wait()
    for p in range(parts):
        x_send(p).start()
    load_x1.wait()

    def head_cols(zt, yy, j):
        h = (zt * 2 + yy) * hp + j
        if padded:
            h = jnp.minimum(h, HEADS - 1)
        return pl.ds(pl.multiple_of(h * D, D), D)

    ones = jnp.ones((PAD, rows), jnp.bfloat16)
    sub8 = lax.broadcasted_iota(jnp.int32, (PAD, D), 0)

    def gram_half(i, half):
        zt = zt_of(i)
        yy = yn if half == 0 else y
        sums = [jnp.zeros((PAD, D), jnp.float32)] * 2
        blocks = [[], []]
        for j in range(hp):
            cols = head_cols(zt, yy, j)
            for k, ref in enumerate((x1, x2)):
                v = ref[:, cols]
                blocks[k].append(pack(dot_tt(v, v)))
                sums[k] = jnp.where(sub8 == j, jnp.dot(ones, v, preferred_element_type=jnp.float32), sums[k])
        for k in range(2):
            store_packed(gp.at[k, zt, yy], blocks[k])
            gp[k, zt, yy, packed_rows(hp) :, :] = sums[k]
        g_d(i, half).start()

    def g_d(i, half):
        zt = zt_of(i)
        yy = yn if half == 0 else y
        return rc(gp.at[1 - c, zt, yy], gd.at[zt, yy], gd_s.at[0], gd_r.at[half, i], core_peer, lay)

    def g_y(i):
        zt = zt_of(i)
        return rc(gp.at[c, zt, yn], gy.at[zt], gy_s.at[0], gy_r.at[i], y_peer, lay)

    def g_z(o, b):
        return rc(gp.at[c, z_xor(o), y], gz.at[o - 1], gz_s.at[0], gz_r.at[o - 1], z_peer(b), lay)

    def g_yph(i):
        zt = zt_of(i)
        g_d(i, 0).wait_recv()
        gp[c, zt, yn] = gp[c, zt, yn] + gd[zt, yn]
        g_y(i).start()

    def g_zph(i):
        zt = zt_of(i)
        o = R - 1 - i
        g_d(i, 1).wait_recv()
        g_y(i).wait_recv()
        terms = terms_of(o) if o else []
        for b in terms:
            g_z(o + b, b).wait_recv()
        total = gp[c, zt, y] + gd[zt, y] + gy[zt]
        for b in terms:
            total = total + gz[o + b - 1]
        gp[c, zt, y] = total
        if o:
            g_z(o, lowest(o)).start()

    def first_body(i, carry):
        gram_half(i, 0)

        @pl.when(i >= 1)
        def _():
            g_yph(i - 1)

        return carry

    def second_body(i, carry):
        gram_half(i, 1)

        @pl.when(i == 0)
        def _():
            g_yph(R - 1)

        return carry

    lax.fori_loop(0, R, first_body, 0)

    def c_d(k, i, half):
        zt = ct_of(i)
        yy = yn if half == 0 else y
        return rc(cp.at[k, zt, yy], cd.at[zt, yy], cd_s.at[0], cd_r.at[half, i], core_peer, lay)

    def own_heads(k):
        return pl.ds(zf, hp - zf) if k == 0 else pl.ds(0, hp)

    def c_y(k, i):
        zt = ct_of(i)
        hs = own_heads(k)
        return rc(cp.at[k, zt, yn, hs], cy.at[zt, hs], cy_s.at[0], cy_r.at[i], y_peer, lay)

    def c_z(k, zt, slot):
        hs = own_heads(k)
        return rc(cp.at[k, zt, y, hs], cz.at[slot, hs], cz_s.at[0], cz_r.at[slot], z_peer_at(z + hop(zt)), lay)

    def c_z_in(k, slot):
        hs = own_heads(k)
        return rc(cp.at[k, z, y, hs], cz.at[slot, hs], cz_s.at[0], cz_r.at[slot], me, other)

    def f_z(zt, slot):
        return rc(
            cp.at[0, zt, :, pl.ds(0, zf)], czf.at[slot], fz_s.at[0], fz_r.at[slot], z_peer_at(z + hop(zt)), lay
        )

    def f_z_in(slot):
        return rc(cp.at[0, z, :, pl.ds(0, zf)], czf.at[slot], fz_s.at[0], fz_r.at[slot], me, other)

    def f_y():
        return rc(cp.at[0, z, yn, pl.ds(0, zf)], cyf, fy_s.at[0], fy_r.at[0], y_peer, lay)

    def sources(zt, own, body):
        if own:
            pl.when(z > 0)(lambda: body(z))
            pl.when(z < R - 1)(lambda: body(R))
        else:
            pl.when(has_source(zt) == 1)(lambda: body(zt))

    def first_z(i, chained=None):
        ready = c == 1
        if chained is not None:
            ready = jnp.logical_and(ready, has_source(ct_of(i)) == chained)

        @pl.when(ready)
        def _():
            own = i == R - 1
            zt = ct_of(i)

            def add(slot):
                f_z_in(slot).wait_recv()
                for half in range(2):
                    for j in range(zf):
                        cp[0, zt, half, j] = cp[0, zt, half, j] + czf[slot, half, j]

            sources(zt, own, add)
            if own:
                f_y().start()
            else:
                f_z(zt, slot_of(zt)).start()

    def cross_half(k, i, half):
        zt = ct_of(i)
        yy = yn if half == 0 else y
        ref = x2 if k == 0 else x2o
        for j in range(hp):
            cols = head_cols(zt, yy, j)
            cp[k, zt, yy, j] = dot_tt(x1[:, cols], ref[:, cols])

        @pl.when(c == k)
        def _():
            c_d(k, i, half).start()

    def cross_y(k, i):
        @pl.when(c == 1 - k)
        def _():
            zt = ct_of(i)
            c_d(k, i, 0).wait_recv()
            for j in range(hp):
                cp[k, zt, yn, j] = cp[k, zt, yn, j] + cd[zt, yn, j]
            c_y(k, i).start()
            if k == 0:
                c_d(k, i, 1).wait_recv()
                for j in range(hp):
                    cp[k, zt, y, j] = cp[k, zt, y, j] + cd[zt, y, j]

    def cross_z(k, i, chained):
        @pl.when(jnp.logical_and(c == 1 - k, has_source(ct_of(i)) == chained))
        def _():
            zt = ct_of(i)
            if k == 1:
                c_d(k, i, 1).wait_recv()
            c_y(k, i).wait_recv()
            for j in range(zf if k == 0 else 0, hp):
                total = cp[k, zt, y, j] + cy[zt, j]
                if k == 1:
                    total = total + cd[zt, y, j]
                cp[k, zt, y, j] = total

            def add(slot):
                c_z_in(k, slot).wait_recv()
                for j in range(zf if k == 0 else 0, hp):
                    cp[k, zt, y, j] = cp[k, zt, y, j] + cz[slot, j]

            sources(zt, False, add)
            c_z(k, zt, slot_of(zt)).start()

    def loop(body, lo, hi):
        def step(i, carry):
            body(i)
            return carry

        lax.fori_loop(lo, hi, step, 0)

    def cross_own(i):
        cross_half(0, i, 0)
        cross_half(0, i, 1)

    def cross_other(i, half):
        p = 2 * i + half
        if p < parts:
            x_send(p).wait_recv()
        cross_half(1, i, half)

    cross_own(0)
    lax.fori_loop(0, R, second_body, 0)
    cross_y(0, 0)
    first_z(0, 0)
    loop(cross_own, 1, R)
    g_zph(0)
    loop(lambda i: cross_y(0, i), 1, R)
    for i in range(1, R - 1):
        g_zph(i)
        if i == 1:
            first_z(0, 1)
            first_z(1, 0)
    cross_other(0, 0)
    cross_other(0, 1)
    g_zph(R - 1)
    cross_y(1, 0)
    for b in bits:
        g_z(b, b).wait_recv()

    eye = (
        lax.broadcasted_iota(jnp.int32, (D, D), 0) == lax.broadcasted_iota(jnp.int32, (D, D), 1)
    ).astype(jnp.float32)
    scales = []
    tail = slice(packed_rows(hp), packed_rows(hp) + PAD)
    col_sums = gp[c, z, y, tail, :]
    for b in bits:
        col_sums = col_sums + gz[b - 1, tail, :]
    for j in range(hp):
        def read(lo, hi):
            total = gp[c, z, y, lo:hi, :]
            for b in bits:
                total = total + gz[b - 1, lo:hi, :]
            return total

        mean = jnp.where(sub8 == 0, col_sums[j : j + 1, :], 0.0) / token_total
        slab[0, j, D:, :] = mean
        cov = load_packed(read, hp, j) / token_total - dot_tt(mean, mean, HI) + ridge_weight * eye
        norm2 = jnp.sum(jnp.sum(cov * cov, axis=1, keepdims=True), axis=0, keepdims=True)
        scale = jnp.sqrt(norm2)
        scales.append(scale)
        y0 = cov / scale
        f = 1.5 * eye - 0.5 * y0
        yb[j] = mm(y0, f)
        zb[j] = f

    def ns_body(t, carry):
        fs = [1.5 * eye - 0.5 * mm(zb[j], yb[j]) for j in range(hp)]
        for j in range(hp):
            yb[j] = mm(yb[j], fs[j])
            zb[j] = mm(fs[j], zb[j])
        return carry

    lax.fori_loop(1, ITERS - 1, ns_body, 0)
    factors = []
    for j in range(hp):
        f = 1.5 * eye - 0.5 * mm(zb[j], yb[j])
        w = mm(f, zb[j]) / jnp.sqrt(scales[j])
        slab[0, j, :D, :] = w
        out[c, z, y, j] = w
        factors.append(pack(w))
    store_packed(wbuf.at[c, z, y], factors)

    def up(d):
        block = wbuf.at[c, z - d, y]
        return rc(block, block, az_s.at[0, d], az_r.at[0, d], z_peer_at(z + 1), lay)

    def down(d):
        block = wbuf.at[c, z + d, y]
        return rc(block, block, az_s.at[1, d], az_r.at[1, d], z_peer_at(z - 1), lay)

    def from_below(d):
        block = wbuf.at[c, z - d, y]
        return rc(block, block, az_s.at[0, d - 1], az_r.at[0, d - 1], z_peer_at(z - 1), lay)

    def from_above(d):
        block = wbuf.at[c, z + d, y]
        return rc(block, block, az_s.at[1, d - 1], az_r.at[1, d - 1], z_peer_at(z + 1), lay)

    def a_y(zs):
        block = wbuf.at[c, zs, y]
        return rc(block, block, ay_s.at[0], ay_r.at[zs], y_peer, lay)

    def a_y_in(zs):
        block = wbuf.at[c, zs, yn]
        return rc(block, block, ay_s.at[0], ay_r.at[zs], y_peer, lay)

    def a_d(cc, zs, half):
        block = wbuf.at[cc, zs, yn if half == 0 else y]
        return rc(block, block, ad_s.at[0], ad_r.at[half, zs], core_peer, lay)

    to_core = rc(slab.at[0], slab.at[1], p_s.at[0], p_r.at[0], core_peer, lay)
    to_lay = [
        rc(wbuf.at[1, z, y], wlay, q_s.at[0], q_r.at[0], core_peer, other),
        rc(slab.at[0, :, pl.ds(D, PAD)], slab.at[2, :, pl.ds(D, PAD)], q_s.at[1], q_r.at[1], core_peer, other),
    ]

    def has_below(d):
        return z - d >= 0

    def has_above(d):
        return z + d < R

    def when(cond):
        return pl.when(cond)

    @when(has_above(1))
    def _():
        up(0).start()

    @when(has_below(1))
    def _():
        down(0).start()

    a_y(z).start()
    to_core.start()
    a_d(c, z, 1).start()

    @pl.when(c == 1)
    def _():
        to_lay[1].start()
        to_lay[0].start()

    def gather_z(d):
        @when(has_below(d))
        def _():
            from_below(d).wait_recv()

            @when(has_above(1))
            def _():
                up(d).start()

            a_y(z - d).start()
            a_d(c, z - d, 1).start()

        @when(has_above(d))
        def _():
            from_above(d).wait_recv()

            @when(has_below(1))
            def _():
                down(d).start()

            a_y(z + d).start()
            a_d(c, z + d, 1).start()

    def expand(cc, zs, yy):
        for j in range(hp):
            out[cc, zs, yy, j] = load_packed(lambda lo, hi: wbuf[cc, zs, yy, lo:hi, :], hp, j)

    def sides(d, body):
        if d == 0:
            body(z)
            return

        @when(has_below(d))
        def _():
            body(z - d)

        @when(has_above(d))
        def _():
            body(z + d)

    def expand_z(d):
        sides(d, lambda zs: expand(c, zs, y))

    def gather_y(d):
        def body(zs):
            a_y_in(zs).wait_recv()
            a_d(c, zs, 0).start()
            expand(c, zs, yn)

        sides(d, body)

    def gather_core(d, half):
        def body(zs):
            a_d(1 - c, zs, half).wait_recv()
            expand(1 - c, zs, yn if half == 0 else y)

        sides(d, body)

    group = (z * 2 + y) * hp
    lane = lax.broadcasted_iota(jnp.int32, sbuf.shape[1:], 1)

    def s_out(k):
        return rc(sbuf.at[me], sbuf.at[me], ss_s.at[0], ss_r.at[0], lax.rem(me + k, n), lay)

    def final(k):
        left_at, right_at = (1, 0) if k == 0 else (0, 2)

        @pl.when(c == 1 - k)
        def _():
            to_core.wait_recv()
            if k == 0:
                f_y().wait_recv()
            else:
                for d in to_lay[::-1]:
                    d.wait_recv()
                for j in range(hp):
                    slab[2, j, :D, :] = load_packed(lambda lo, hi: wlay[lo:hi, :], hp, j)
            c_y(k, R - 1).wait_recv()

            def add(slot):
                c_z_in(k, slot).wait_recv()
                for j in range(zf if k == 0 else 0, hp):
                    cp[k, z, y, j] = cp[k, z, y, j] + cz[slot, j]

            sources(z, True, add)
            for j in range(hp):
                left = slab[left_at, j]
                right = slab[right_at, j]
                if k == 0 and j < zf:
                    total = cp[k, z, y, j] + cyf[j]
                else:
                    total = cp[k, z, y, j] + cy[z, j]
                zb[j] = total / token_total - dot_tt(left[D:, :], right[D:, :], HI)
            if k == 1:
                c_d(k, R - 1, 1).wait_recv()
                for j in range(hp):
                    zb[j] = zb[j] + cd[z, y, j] / token_total
            for j in range(hp):
                yb[j] = mm(slab[left_at, j, :D, :], zb[j])
            for j in range(hp):
                white = mm(yb[j], slab[right_at, j, :D, :])
                zb[j] = white * white
            tile = jnp.zeros(sbuf.shape[1:], jnp.float32)
            for j in range(hp):
                value = jnp.sum(jnp.sum(zb[j], axis=0, keepdims=True), axis=1, keepdims=True) / HEAD_DIM
                tile = jnp.where(lane == group + j, value, tile)
            sbuf[me] = tile
            for q in range(1, n):
                s_out(q).start()

    for i in range(R - 1):
        cross_z(0, i, 0)
    for i in range(1, R - 1):
        first_z(i, 1)
        if i + 1 < R - 1:
            first_z(i + 1, 0)
    cross_z(1, 0, 0)
    cross_other(1, 0)
    cross_other(1, 1)
    cross_y(1, 1)
    gather_z(1)
    for d in range(2, R - 1):
        cross_other(d, 0)
        cross_y(1, d)
        gather_y(d - 2)
        gather_z(d)
        cross_other(d, 1)
        for q in range(d - 2, R - 1 if d == R - 2 else d - 1):
            cross_z(0, q, 1)
        cross_z(1, d - 2, 1)
        cross_z(1, d - 1, 0)
        expand_z(d - 1)
    gather_z(R - 1)
    cross_z(1, R - 2, 0)
    gather_y(R - 3)
    cross_other(R - 1, 0)
    cross_y(1, R - 1)
    cross_z(1, R - 3, 1)
    cross_z(1, R - 2, 1)
    first_z(R - 1)
    gather_y(R - 2)
    expand_z(R - 2)
    expand_z(R - 1)
    for d in range(R - 1):
        gather_core(d, 1)
    cross_other(R - 1, 1)
    final(0)
    final(1)
    gather_y(R - 1)
    gather_core(R - 1, 1)
    for d in range(R):
        gather_core(d, 0)

    def sent(ref, sem):
        rc(ref, ref, sem.at[0], sem.at[0], core_peer, lay).wait_send()

    sent(x2, x_s)
    sent(gd, gd_s)
    sent(gy, gy_s)
    sent(gz, gz_s)
    sent(cd, cd_s)
    sent(wbuf.at[c, :, y], ay_s)
    sent(wbuf.at[c], ad_s)
    for k in range(2):
        @pl.when(c == 1 - k)
        def _():
            hs = own_heads(k)
            sent(cy.at[:, hs], cy_s)
            sent(cz.at[pl.ds(0, R - 1), hs], cz_s)
            if k == 0:
                sent(czf.at[pl.ds(0, R - 1)], fz_s)
                f_y().wait_send()

    for d in range(R - 1):
        @when(jnp.logical_and(has_below(d), has_above(1)))
        def _():
            up(d).wait_send()

        @when(jnp.logical_and(has_above(d), has_below(1)))
        def _():
            down(d).wait_send()

    to_core.wait_send()

    @pl.when(c == 1)
    def _():
        for d in to_lay:
            d.wait_send()

    tiles = sbuf.at[pl.ds(0, n - 1)]
    sent(tiles, ss_s)
    rc(tiles, tiles, ss_s.at[0], ss_r.at[0], core_peer, lay).wait_recv()
    row0 = sbuf[0]
    row1 = sbuf[1]
    for i in range(2, n, 2):
        row0 = row0 + sbuf[i]
        row1 = row1 + sbuf[i + 1]
    sub = lax.broadcasted_iota(jnp.int32, row0.shape, 0)
    simout[...] = jnp.where(sub == lay, row1, row0)[:2, :HEADS]


def write_out(white, sims, white_out, sims_out, sem):
    copies = [pltpu.make_async_copy(sims, sims_out, sem.at[0])]
    for k in range(2):
        for i in range(white.shape[1]):
            copies.append(pltpu.make_async_copy(white.at[k, i], white_out.at[k, i], sem.at[len(copies)]))
    for d in copies:
        d.start()
    for d in copies:
        d.wait()


def solution(mesh):
    n = mesh.shape["tok"]
    R = n // 4
    hp = -(-HEADS // (n // 2))
    zf = max(hp * Z_FIRST // 5, 1)
    D = HEAD_DIM
    E = packed_rows(hp) + PAD
    parts = 1 if R * 2 * hp != HEADS else 2 * R

    def local(first_acts, second_acts):
        _, rows, width = first_acts.shape
        token_total = float(rows * n)
        f32 = jnp.float32
        bf16 = jnp.bfloat16
        dma = lambda *k: pltpu.SemaphoreType.DMA(tuple(max(q, 1) for q in k))
        out, sims = pl.pallas_call(
            functools.partial(kernel, n, R, hp, zf, token_total),
            out_shape=(
                pltpu.VMEM((2, R, 2, hp, D, D), f32),
                pltpu.VMEM((2, HEADS), f32),
            ),
            in_specs=[pl.BlockSpec(memory_space=pltpu.MemorySpace.HBM)] * 2,
            out_specs=(
                pl.BlockSpec(memory_space=pltpu.VMEM),
                pl.BlockSpec(memory_space=pltpu.VMEM),
            ),
            scratch_shapes=[
                pltpu.VMEM((rows, width), bf16),
                pltpu.VMEM((rows, width), bf16),
                pltpu.VMEM((rows, width), bf16),
                pltpu.VMEM((2, R, 2, E, D), f32),
                pltpu.VMEM((R, 2, E, D), f32),
                pltpu.VMEM((R, E, D), f32),
                pltpu.VMEM((R - 1, E, D), f32),
                pltpu.VMEM((2, R, 2, hp, D, D), f32),
                pltpu.VMEM((R, 2, hp, D, D), f32),
                pltpu.VMEM((R, hp, D, D), f32),
                pltpu.VMEM((R + 1, hp, D, D), f32),
                pltpu.VMEM((zf, D, D), f32),
                pltpu.VMEM((R + 1, 2, zf, D, D), f32),
                pltpu.VMEM((3, hp, D + PAD, D), f32),
                pltpu.VMEM((E - PAD, D), f32),
                pltpu.VMEM((2, R, 2, E - PAD, D), f32),
                pltpu.VMEM((n, 8, D), f32),
                pltpu.VMEM((hp, D, D), f32),
                pltpu.VMEM((hp, D, D), f32),
                dma(2), dma(1), dma(parts),
                dma(1), dma(2, R), dma(1), dma(R), dma(1), dma(R - 1),
                dma(1), dma(2, R), dma(1), dma(R), dma(1), dma(R + 1),
                dma(1), dma(1), dma(1), dma(R + 1),
                dma(1), dma(1), dma(2), dma(2),
                dma(2, R - 1), dma(2, R - 1), dma(1), dma(R), dma(1), dma(2, R),
                dma(1), dma(1),
            ],
            compiler_params=pltpu.CompilerParams(
                collective_id=0, has_side_effects=True, vmem_limit_bytes=VMEM_LIMIT
            ),
        )(first_acts[0], second_acts[0])
        out, sims = pl.pallas_call(
            write_out,
            out_shape=(
                jax.ShapeDtypeStruct((2, R, 2, hp, D, D), f32),
                jax.ShapeDtypeStruct((2, HEADS), f32),
            ),
            in_specs=[pl.BlockSpec(memory_space=pl.ANY)] * 2,
            out_specs=(pl.BlockSpec(memory_space=pltpu.MemorySpace.HBM),) * 2,
            scratch_shapes=[dma(2 * R + 1)],
            compiler_params=pltpu.CompilerParams(vmem_limit_bytes=1024 * 1024),
        )(out, sims)
        whitening = out.reshape(2, R * 2 * hp, D, D)[:, None, :HEADS]
        return whitening, sims[None]

    in_specs = (P("lay", "tok", None), P("lay", "tok", None))
    out_specs = (P(None, "lay", None, None, None), P("lay", None, None))
    return jax.shard_map(local, mesh=mesh, in_specs=in_specs, out_specs=out_specs, check_vma=False)
```

```python
import functools

import jax
import jax.numpy as jnp
from jax import lax
from jax.experimental import pallas as pl
from jax.experimental.pallas import tpu as pltpu
from jax.sharding import PartitionSpec as P

HEADS = 40
HEAD_DIM = 128
ITERS = 6
PAD = 8

ridge_weight = 0.05
Z_FIRST = 2
VMEM_LIMIT = 54 * 1024 * 1024
MESH = pl.DeviceIdType.MESH
HI = lax.Precision.HIGHEST


def dot_tt(a, b, precision=None):
    return lax.dot_general(
        a, b, (((0,), (0,)), ((), ())), preferred_element_type=jnp.float32, precision=precision
    )


def mm(a, b):
    return jnp.dot(a, b, preferred_element_type=jnp.float32, precision=HI)


BLOCKS = HEAD_DIM // 8
KEPT = BLOCKS // 2 + 1
MAIN = 8 * (KEPT - 1)


def lane_block():
    return lax.broadcasted_iota(jnp.int32, (8, HEAD_DIM), 1) // 8


def pack(a):
    lb = lane_block()
    xs = [a[8 * e : 8 * e + 8, :] for e in range(BLOCKS)]
    step = 1
    while step < BLOCKS:
        bit = (lb // step) % 2 == 1
        xs = [jnp.where(bit, xs[(e + step) % BLOCKS], xs[e]) for e in range(BLOCKS)]
        step *= 2
    return jnp.concatenate([xs[(-d) % BLOCKS] for d in range(KEPT)], axis=0)


def packed_rows(hp):
    return hp * MAIN + (hp + 1) // 2 * 8


def store_packed(ref, blocks):
    hp = len(blocks)
    first = lax.broadcasted_iota(jnp.int32, (8, HEAD_DIM), 1) < HEAD_DIM // 2
    for j in range(hp):
        ref[j * MAIN : (j + 1) * MAIN, :] = blocks[j][:MAIN, :]
    for t in range((hp + 1) // 2):
        left, right = blocks[2 * t], blocks[min(2 * t + 1, hp - 1)]
        ref[hp * MAIN + 8 * t : hp * MAIN + 8 * t + 8, :] = jnp.where(first, left[MAIN:, :], right[MAIN:, :])


def load_packed(read, hp, j):
    at = hp * MAIN + 8 * (j // 2)
    return unpack(jnp.concatenate([read(j * MAIN, (j + 1) * MAIN), read(at, at + 8)], axis=0), j % 2)


def unpack(p, odd):
    lb = lane_block()
    zero = jnp.zeros((8, HEAD_DIM), jnp.float32)
    ys = [zero] * BLOCKS
    for d in range(KEPT):
        ys[(-d) % BLOCKS] = p[8 * d : 8 * d + 8, :]
    step = 1
    while step < BLOCKS:
        bit = (lb // step) % 2 == 1
        ys = [jnp.where(bit, ys[(e - step) % BLOCKS], ys[e]) for e in range(BLOCKS)]
        step *= 2
    half = jnp.concatenate(ys, axis=0)
    rb = lax.broadcasted_iota(jnp.int32, (HEAD_DIM, HEAD_DIM), 0) // 8
    cb = lax.broadcasted_iota(jnp.int32, (HEAD_DIM, HEAD_DIM), 1) // 8
    away = (cb - rb + BLOCKS) % BLOCKS
    side = cb >= BLOCKS // 2 if odd else cb < BLOCKS // 2
    keep = jnp.logical_or(away < KEPT - 1, jnp.logical_and(away == KEPT - 1, side))
    return jnp.where(keep, half, half.T)


def kernel(
    n, R, hp, zf, token_total,
    x1h, x2h, out, simout,
    x1, x2, x2o, gp, gd, gy, gz, cp, cd, cy, cz, cyf, czf, slab, wlay, wbuf, sbuf, yb, zb,
    l_s, x_s, x_r, gd_s, gd_r, gy_s, gy_r, gz_s, gz_r,
    cd_s, cd_r, cy_s, cy_r, cz_s, cz_r, fy_s, fy_r, fz_s, fz_r,
    p_s, p_r, q_s, q_r, az_s, az_r, ay_s, ay_r, ad_s, ad_r, ss_s, ss_r,
):
    me = lax.axis_index("tok")
    lay = lax.axis_index("lay")
    other = 1 - lay
    c = lax.rem(me, 2)
    y = lax.rem(me // 2, 2)
    z = me // 4
    yn = 1 - y
    rows = x1.shape[0]
    D = HEAD_DIM
    core_peer = z * 4 + y * 2 + (1 - c)
    y_peer = z * 4 + yn * 2 + c
    padded = R * 2 * hp != HEADS

    bits = [1 << t for t in range(R.bit_length() - 1)]

    def z_xor(o):
        total = 0
        for b in bits:
            zb = lax.rem(z // b, 2)
            ob = lax.rem(o // b, 2) if not isinstance(o, int) else o // b % 2
            total = total + b * (zb + ob - 2 * zb * ob)
        return total

    def z_peer_at(zt):
        return zt * 4 + y * 2 + c

    def z_peer(o):
        return z_xor(o) * 4 + y * 2 + c

    def at_least(a, b):
        return (a - b + R) // R

    def ct_of(i):
        step = R - 1 - i
        below = z
        above = R - 1 - z
        short = jnp.minimum(below, above)
        up_far = at_least(above, below)
        paired = 1 - at_least(step, 2 * short + 1)
        dist = paired * ((step + 1) // 2) + (1 - paired) * (step - short)
        near_side = paired * (1 - lax.rem(step, 2))
        up = up_far + near_side - 2 * up_far * near_side
        return z + dist * (2 * up - 1)

    def hop(zt):
        return 2 * at_least(zt, z) - 1

    def slot_of(zt):
        direction = hop(zt)
        last = (R - direction * (zt - z)) // (R - 1)
        down = (1 - direction) // 2
        return zt + (R - zt) * last * down

    def has_source(zt):
        return inside(z - hop(zt))

    def inside(q):
        return at_least(q, 0) * at_least(R - 1, q)

    def terms_of(o):
        return [b for b in bits if o % (2 * b) == 0]

    def lowest(o):
        return next(b for b in bits if o // b % 2)

    def rc(src, dst, s, r, tok, ly):
        return pltpu.make_async_remote_copy(
            src_ref=src, dst_ref=dst, send_sem=s, recv_sem=r,
            device_id=(tok, ly), device_id_type=MESH,
        )

    def zt_of(i):
        return z_xor(R - 1 - i)

    barrier = pltpu.get_barrier_semaphore()
    for k in range(1, n):
        pl.semaphore_signal(barrier, inc=1, device_id=(lax.rem(me + k, n), lay), device_id_type=MESH)
    pl.semaphore_signal(barrier, inc=1, device_id=(me, other), device_id_type=MESH)

    parts = 1 if padded else 2 * R
    width = x1.shape[1] // parts

    def part_cols(p):
        if padded:
            return pl.ds(0, width)
        half = yn if p % 2 == 0 else y
        return pl.ds(pl.multiple_of((ct_of(p // 2) * 2 + half) * width, 128), width)

    load_x2 = pltpu.make_async_copy(x2h, x2, l_s.at[0])
    load_x1 = pltpu.make_async_copy(x1h, x1, l_s.at[1])
    load_x2.start()
    load_x1.start()

    def x_send(p):
        cols = part_cols(p)
        return rc(x2.at[:, cols], x2o.at[:, cols], x_s.at[0], x_r.at[p], me, other)

    pl.semaphore_wait(barrier, n)
    load_x2.wait()
    for p in range(parts):
        x_send(p).start()
    load_x1.wait()

    def head_cols(zt, yy, j):
        h = (zt * 2 + yy) * hp + j
        if padded:
            h = jnp.minimum(h, HEADS - 1)
        return pl.ds(pl.multiple_of(h * D, D), D)

    ones = jnp.ones((PAD, rows), jnp.bfloat16)
    sub8 = lax.broadcasted_iota(jnp.int32, (PAD, D), 0)

    def gram_half(i, half):
        zt = zt_of(i)
        yy = yn if half == 0 else y
        sums = [jnp.zeros((PAD, D), jnp.float32)] * 2
        blocks = [[], []]
        for j in range(hp):
            cols = head_cols(zt, yy, j)
            for k, ref in enumerate((x1, x2)):
                v = ref[:, cols]
                blocks[k].append(pack(dot_tt(v, v)))
                sums[k] = jnp.where(sub8 == j, jnp.dot(ones, v, preferred_element_type=jnp.float32), sums[k])
        for k in range(2):
            store_packed(gp.at[k, zt, yy], blocks[k])
            gp[k, zt, yy, packed_rows(hp) :, :] = sums[k]
        g_d(i, half).start()

    def g_d(i, half):
        zt = zt_of(i)
        yy = yn if half == 0 else y
        return rc(gp.at[1 - c, zt, yy], gd.at[zt, yy], gd_s.at[0], gd_r.at[half, i], core_peer, lay)

    def g_y(i):
        zt = zt_of(i)
        return rc(gp.at[c, zt, yn], gy.at[zt], gy_s.at[0], gy_r.at[i], y_peer, lay)

    def g_z(o, b):
        return rc(gp.at[c, z_xor(o), y], gz.at[o - 1], gz_s.at[0], gz_r.at[o - 1], z_peer(b), lay)

    def g_yph(i):
        zt = zt_of(i)
        g_d(i, 0).wait_recv()
        gp[c, zt, yn] = gp[c, zt, yn] + gd[zt, yn]
        g_y(i).start()

    def g_zph(i):
        zt = zt_of(i)
        o = R - 1 - i
        g_d(i, 1).wait_recv()
        g_y(i).wait_recv()
        terms = terms_of(o) if o else []
        for b in terms:
            g_z(o + b, b).wait_recv()
        total = gp[c, zt, y] + gd[zt, y] + gy[zt]
        for b in terms:
            total = total + gz[o + b - 1]
        gp[c, zt, y] = total
        if o:
            g_z(o, lowest(o)).start()

    def first_body(i, carry):
        gram_half(i, 0)

        @pl.when(i >= 1)
        def _():
            g_yph(i - 1)

        return carry

    def second_body(i, carry):
        gram_half(i, 1)

        @pl.when(i == 0)
        def _():
            g_yph(R - 1)

        return carry

    lax.fori_loop(0, R, first_body, 0)

    def c_d(k, i, half):
        zt = ct_of(i)
        yy = yn if half == 0 else y
        return rc(cp.at[k, zt, yy], cd.at[zt, yy], cd_s.at[0], cd_r.at[half, i], core_peer, lay)

    def own_heads(k):
        return pl.ds(zf, hp - zf) if k == 0 else pl.ds(0, hp)

    def c_y(k, i):
        zt = ct_of(i)
        hs = own_heads(k)
        return rc(cp.at[k, zt, yn, hs], cy.at[zt, hs], cy_s.at[0], cy_r.at[i], y_peer, lay)

    def c_z(k, zt, slot):
        hs = own_heads(k)
        return rc(cp.at[k, zt, y, hs], cz.at[slot, hs], cz_s.at[0], cz_r.at[slot], z_peer_at(z + hop(zt)), lay)

    def c_z_in(k, slot):
        hs = own_heads(k)
        return rc(cp.at[k, z, y, hs], cz.at[slot, hs], cz_s.at[0], cz_r.at[slot], me, other)

    def f_z(zt, slot):
        return rc(
            cp.at[0, zt, :, pl.ds(0, zf)], czf.at[slot], fz_s.at[0], fz_r.at[slot], z_peer_at(z + hop(zt)), lay
        )

    def f_z_in(slot):
        return rc(cp.at[0, z, :, pl.ds(0, zf)], czf.at[slot], fz_s.at[0], fz_r.at[slot], me, other)

    def f_y():
        return rc(cp.at[0, z, yn, pl.ds(0, zf)], cyf, fy_s.at[0], fy_r.at[0], y_peer, lay)

    def sources(zt, own, body):
        if own:
            pl.when(z > 0)(lambda: body(z))
            pl.when(z < R - 1)(lambda: body(R))
        else:
            pl.when(has_source(zt) == 1)(lambda: body(zt))

    def first_z(i, chained=None):
        ready = c == 1
        if chained is not None:
            ready = jnp.logical_and(ready, has_source(ct_of(i)) == chained)

        @pl.when(ready)
        def _():
            own = i == R - 1
            zt = ct_of(i)

            def add(slot):
                f_z_in(slot).wait_recv()
                for half in range(2):
                    for j in range(zf):
                        cp[0, zt, half, j] = cp[0, zt, half, j] + czf[slot, half, j]

            sources(zt, own, add)
            if own:
                f_y().start()
            else:
                f_z(zt, slot_of(zt)).start()

    def cross_half(k, i, half):
        zt = ct_of(i)
        yy = yn if half == 0 else y
        ref = x2 if k == 0 else x2o
        for j in range(hp):
            cols = head_cols(zt, yy, j)
            cp[k, zt, yy, j] = dot_tt(x1[:, cols], ref[:, cols])

        @pl.when(c == k)
        def _():
            c_d(k, i, half).start()

    def cross_y(k, i):
        @pl.when(c == 1 - k)
        def _():
            zt = ct_of(i)
            c_d(k, i, 0).wait_recv()
            for j in range(hp):
                cp[k, zt, yn, j] = cp[k, zt, yn, j] + cd[zt, yn, j]
            c_y(k, i).start()
            if k == 0:
                c_d(k, i, 1).wait_recv()
                for j in range(hp):
                    cp[k, zt, y, j] = cp[k, zt, y, j] + cd[zt, y, j]

    def cross_z(k, i, chained):
        @pl.when(jnp.logical_and(c == 1 - k, has_source(ct_of(i)) == chained))
        def _():
            zt = ct_of(i)
            if k == 1:
                c_d(k, i, 1).wait_recv()
            c_y(k, i).wait_recv()
            for j in range(zf if k == 0 else 0, hp):
                total = cp[k, zt, y, j] + cy[zt, j]
                if k == 1:
                    total = total + cd[zt, y, j]
                cp[k, zt, y, j] = total

            def add(slot):
                c_z_in(k, slot).wait_recv()
                for j in range(zf if k == 0 else 0, hp):
                    cp[k, zt, y, j] = cp[k, zt, y, j] + cz[slot, j]

            sources(zt, False, add)
            c_z(k, zt, slot_of(zt)).start()

    def loop(body, lo, hi):
        def step(i, carry):
            body(i)
            return carry

        lax.fori_loop(lo, hi, step, 0)

    def cross_own(i):
        cross_half(0, i, 0)
        cross_half(0, i, 1)

    def cross_other(i, half):
        p = 2 * i + half
        if p < parts:
            x_send(p).wait_recv()
        cross_half(1, i, half)

    cross_own(0)
    lax.fori_loop(0, R, second_body, 0)
    cross_y(0, 0)
    first_z(0, 0)
    loop(cross_own, 1, R)
    g_zph(0)
    loop(lambda i: cross_y(0, i), 1, R)
    for i in range(1, R - 1):
        g_zph(i)
        if i == 1:
            first_z(0, 1)
            first_z(1, 0)
    cross_other(0, 0)
    cross_other(0, 1)
    g_zph(R - 1)
    cross_y(1, 0)
    for b in bits:
        g_z(b, b).wait_recv()

    eye = (
        lax.broadcasted_iota(jnp.int32, (D, D), 0) == lax.broadcasted_iota(jnp.int32, (D, D), 1)
    ).astype(jnp.float32)
    scales = []
    tail = slice(packed_rows(hp), packed_rows(hp) + PAD)
    col_sums = gp[c, z, y, tail, :]
    for b in bits:
        col_sums = col_sums + gz[b - 1, tail, :]
    for j in range(hp):
        def read(lo, hi):
            total = gp[c, z, y, lo:hi, :]
            for b in bits:
                total = total + gz[b - 1, lo:hi, :]
            return total

        mean = jnp.where(sub8 == 0, col_sums[j : j + 1, :], 0.0) / token_total
        slab[0, j, D:, :] = mean
        cov = load_packed(read, hp, j) / token_total - dot_tt(mean, mean, HI) + ridge_weight * eye
        norm2 = jnp.sum(jnp.sum(cov * cov, axis=1, keepdims=True), axis=0, keepdims=True)
        scale = jnp.sqrt(norm2)
        scales.append(scale)
        y0 = cov / scale
        f = 1.5 * eye - 0.5 * y0
        yb[j] = mm(y0, f)
        zb[j] = f

    def ns_body(t, carry):
        fs = [1.5 * eye - 0.5 * mm(zb[j], yb[j]) for j in range(hp)]
        for j in range(hp):
            yb[j] = mm(yb[j], fs[j])
            zb[j] = mm(fs[j], zb[j])
        return carry

    lax.fori_loop(1, ITERS - 1, ns_body, 0)
    factors = []
    for j in range(hp):
        f = 1.5 * eye - 0.5 * mm(zb[j], yb[j])
        w = mm(f, zb[j]) / jnp.sqrt(scales[j])
        slab[0, j, :D, :] = w
        out[c, z, y, j] = w
        factors.append(pack(w))
    store_packed(wbuf.at[c, z, y], factors)

    def up(d):
        block = wbuf.at[c, z - d, y]
        return rc(block, block, az_s.at[0, d], az_r.at[0, d], z_peer_at(z + 1), lay)

    def down(d):
        block = wbuf.at[c, z + d, y]
        return rc(block, block, az_s.at[1, d], az_r.at[1, d], z_peer_at(z - 1), lay)

    def from_below(d):
        block = wbuf.at[c, z - d, y]
        return rc(block, block, az_s.at[0, d - 1], az_r.at[0, d - 1], z_peer_at(z - 1), lay)

    def from_above(d):
        block = wbuf.at[c, z + d, y]
        return rc(block, block, az_s.at[1, d - 1], az_r.at[1, d - 1], z_peer_at(z + 1), lay)

    def a_y(zs):
        block = wbuf.at[c, zs, y]
        return rc(block, block, ay_s.at[0], ay_r.at[zs], y_peer, lay)

    def a_y_in(zs):
        block = wbuf.at[c, zs, yn]
        return rc(block, block, ay_s.at[0], ay_r.at[zs], y_peer, lay)

    def a_d(cc, zs, half):
        block = wbuf.at[cc, zs, yn if half == 0 else y]
        return rc(block, block, ad_s.at[0], ad_r.at[half, zs], core_peer, lay)

    to_core = rc(slab.at[0], slab.at[1], p_s.at[0], p_r.at[0], core_peer, lay)
    to_lay = [
        rc(wbuf.at[1, z, y], wlay, q_s.at[0], q_r.at[0], core_peer, other),
        rc(slab.at[0, :, pl.ds(D, PAD)], slab.at[2, :, pl.ds(D, PAD)], q_s.at[1], q_r.at[1], core_peer, other),
    ]

    def has_below(d):
        return z - d >= 0

    def has_above(d):
        return z + d < R

    def when(cond):
        return pl.when(cond)

    @when(has_above(1))
    def _():
        up(0).start()

    @when(has_below(1))
    def _():
        down(0).start()

    a_y(z).start()
    to_core.start()
    a_d(c, z, 1).start()

    @pl.when(c == 1)
    def _():
        to_lay[1].start()
        to_lay[0].start()

    def gather_z(d):
        @when(has_below(d))
        def _():
            from_below(d).wait_recv()

            @when(has_above(1))
            def _():
                up(d).start()

            a_y(z - d).start()
            a_d(c, z - d, 1).start()

        @when(has_above(d))
        def _():
            from_above(d).wait_recv()

            @when(has_below(1))
            def _():
                down(d).start()

            a_y(z + d).start()
            a_d(c, z + d, 1).start()

    def expand(cc, zs, yy):
        for j in range(hp):
            out[cc, zs, yy, j] = load_packed(lambda lo, hi: wbuf[cc, zs, yy, lo:hi, :], hp, j)

    def sides(d, body):
        if d == 0:
            body(z)
            return

        @when(has_below(d))
        def _():
            body(z - d)

        @when(has_above(d))
        def _():
            body(z + d)

    def expand_z(d):
        sides(d, lambda zs: expand(c, zs, y))

    def gather_y(d):
        def body(zs):
            a_y_in(zs).wait_recv()
            a_d(c, zs, 0).start()
            expand(c, zs, yn)

        sides(d, body)

    def gather_core(d, half):
        def body(zs):
            a_d(1 - c, zs, half).wait_recv()
            expand(1 - c, zs, yn if half == 0 else y)

        sides(d, body)

    group = (z * 2 + y) * hp
    lane = lax.broadcasted_iota(jnp.int32, sbuf.shape[1:], 1)

    def s_out(k):
        return rc(sbuf.at[me], sbuf.at[me], ss_s.at[0], ss_r.at[0], lax.rem(me + k, n), lay)

    def final(k):
        left_at, right_at = (1, 0) if k == 0 else (0, 2)

        @pl.when(c == 1 - k)
        def _():
            to_core.wait_recv()
            if k == 0:
                f_y().wait_recv()
            else:
                to_lay[1].wait_recv()
            c_y(k, R - 1).wait_recv()

            def add(slot):
                c_z_in(k, slot).wait_recv()
                for j in range(zf if k == 0 else 0, hp):
                    cp[k, z, y, j] = cp[k, z, y, j] + cz[slot, j]

            sources(z, True, add)
            for j in range(hp):
                left = slab[left_at, j]
                right = slab[right_at, j]
                if k == 0 and j < zf:
                    total = cp[k, z, y, j] + cyf[j]
                else:
                    total = cp[k, z, y, j] + cy[z, j]
                zb[j] = total / token_total - dot_tt(left[D:, :], right[D:, :], HI)
            if k == 1:
                c_d(k, R - 1, 1).wait_recv()
                for j in range(hp):
                    zb[j] = zb[j] + cd[z, y, j] / token_total
            for j in range(hp):
                yb[j] = mm(slab[left_at, j, :D, :], zb[j])
            if k == 1:
                to_lay[0].wait_recv()
                for j in range(hp):
                    slab[2, j, :D, :] = load_packed(lambda lo, hi: wlay[lo:hi, :], hp, j)
            for j in range(hp):
                white = mm(yb[j], slab[right_at, j, :D, :])
                zb[j] = white * white
            tile = jnp.zeros(sbuf.shape[1:], jnp.float32)
            for j in range(hp):
                value = jnp.sum(jnp.sum(zb[j], axis=0, keepdims=True), axis=1, keepdims=True) / HEAD_DIM
                tile = jnp.where(lane == group + j, value, tile)
            sbuf[me] = tile
            for q in range(1, n):
                s_out(q).start()

    for i in range(R - 1):
        cross_z(0, i, 0)
    for i in range(1, R - 1):
        first_z(i, 1)
        if i + 1 < R - 1:
            first_z(i + 1, 0)
    cross_z(1, 0, 0)
    cross_other(1, 0)
    cross_other(1, 1)
    cross_y(1, 1)
    gather_z(1)
    for d in range(2, R - 1):
        cross_other(d, 0)
        cross_y(1, d)
        gather_y(d - 2)
        gather_z(d)
        cross_other(d, 1)
        for q in range(d - 2, R - 1 if d == R - 2 else d - 1):
            cross_z(0, q, 1)
        cross_z(1, d - 2, 1)
        cross_z(1, d - 1, 0)
        expand_z(d - 1)
    gather_z(R - 1)
    cross_z(1, R - 2, 0)
    gather_y(R - 3)
    cross_other(R - 1, 0)
    cross_y(1, R - 1)
    cross_z(1, R - 3, 1)
    cross_z(1, R - 2, 1)
    first_z(R - 1)
    gather_y(R - 2)
    expand_z(R - 2)
    expand_z(R - 1)
    for d in range(R - 1):
        gather_core(d, 1)
    cross_other(R - 1, 1)
    final(0)
    final(1)
    gather_y(R - 1)
    gather_core(R - 1, 1)
    for d in range(R):
        gather_core(d, 0)

    def sent(ref, sem):
        rc(ref, ref, sem.at[0], sem.at[0], core_peer, lay).wait_send()

    sent(x2, x_s)
    sent(gd, gd_s)
    sent(gy, gy_s)
    sent(gz, gz_s)
    sent(cd, cd_s)
    sent(wbuf.at[c, :, y], ay_s)
    sent(wbuf.at[c], ad_s)
    for k in range(2):
        @pl.when(c == 1 - k)
        def _():
            hs = own_heads(k)
            sent(cy.at[:, hs], cy_s)
            sent(cz.at[pl.ds(0, R - 1), hs], cz_s)
            if k == 0:
                sent(czf.at[pl.ds(0, R - 1)], fz_s)
                f_y().wait_send()

    for d in range(R - 1):
        @when(jnp.logical_and(has_below(d), has_above(1)))
        def _():
            up(d).wait_send()

        @when(jnp.logical_and(has_above(d), has_below(1)))
        def _():
            down(d).wait_send()

    to_core.wait_send()

    @pl.when(c == 1)
    def _():
        for d in to_lay:
            d.wait_send()

    tiles = sbuf.at[pl.ds(0, n - 1)]
    sent(tiles, ss_s)
    rc(tiles, tiles, ss_s.at[0], ss_r.at[0], core_peer, lay).wait_recv()
    row0 = sbuf[0]
    row1 = sbuf[1]
    for i in range(2, n, 2):
        row0 = row0 + sbuf[i]
        row1 = row1 + sbuf[i + 1]
    sub = lax.broadcasted_iota(jnp.int32, row0.shape, 0)
    simout[...] = jnp.where(sub == lay, row1, row0)[:2, :HEADS]


def write_out(white, sims, white_out, sims_out, sem):
    copies = [pltpu.make_async_copy(sims, sims_out, sem.at[0])]
    for k in range(2):
        for i in range(white.shape[1]):
            copies.append(pltpu.make_async_copy(white.at[k, i], white_out.at[k, i], sem.at[len(copies)]))
    for d in copies:
        d.start()
    for d in copies:
        d.wait()


def solution(mesh):
    n = mesh.shape["tok"]
    R = n // 4
    hp = -(-HEADS // (n // 2))
    zf = max(hp * Z_FIRST // 5, 1)
    D = HEAD_DIM
    E = packed_rows(hp) + PAD
    parts = 1 if R * 2 * hp != HEADS else 2 * R

    def local(first_acts, second_acts):
        _, rows, width = first_acts.shape
        token_total = float(rows * n)
        f32 = jnp.float32
        bf16 = jnp.bfloat16
        dma = lambda *k: pltpu.SemaphoreType.DMA(tuple(max(q, 1) for q in k))
        out, sims = pl.pallas_call(
            functools.partial(kernel, n, R, hp, zf, token_total),
            out_shape=(
                pltpu.VMEM((2, R, 2, hp, D, D), f32),
                pltpu.VMEM((2, HEADS), f32),
            ),
            in_specs=[pl.BlockSpec(memory_space=pltpu.MemorySpace.HBM)] * 2,
            out_specs=(
                pl.BlockSpec(memory_space=pltpu.VMEM),
                pl.BlockSpec(memory_space=pltpu.VMEM),
            ),
            scratch_shapes=[
                pltpu.VMEM((rows, width), bf16),
                pltpu.VMEM((rows, width), bf16),
                pltpu.VMEM((rows, width), bf16),
                pltpu.VMEM((2, R, 2, E, D), f32),
                pltpu.VMEM((R, 2, E, D), f32),
                pltpu.VMEM((R, E, D), f32),
                pltpu.VMEM((R - 1, E, D), f32),
                pltpu.VMEM((2, R, 2, hp, D, D), f32),
                pltpu.VMEM((R, 2, hp, D, D), f32),
                pltpu.VMEM((R, hp, D, D), f32),
                pltpu.VMEM((R + 1, hp, D, D), f32),
                pltpu.VMEM((zf, D, D), f32),
                pltpu.VMEM((R + 1, 2, zf, D, D), f32),
                pltpu.VMEM((3, hp, D + PAD, D), f32),
                pltpu.VMEM((E - PAD, D), f32),
                pltpu.VMEM((2, R, 2, E - PAD, D), f32),
                pltpu.VMEM((n, 8, D), f32),
                pltpu.VMEM((hp, D, D), f32),
                pltpu.VMEM((hp, D, D), f32),
                dma(2), dma(1), dma(parts),
                dma(1), dma(2, R), dma(1), dma(R), dma(1), dma(R - 1),
                dma(1), dma(2, R), dma(1), dma(R), dma(1), dma(R + 1),
                dma(1), dma(1), dma(1), dma(R + 1),
                dma(1), dma(1), dma(2), dma(2),
                dma(2, R - 1), dma(2, R - 1), dma(1), dma(R), dma(1), dma(2, R),
                dma(1), dma(1),
            ],
            compiler_params=pltpu.CompilerParams(
                collective_id=0, has_side_effects=True, vmem_limit_bytes=VMEM_LIMIT
            ),
        )(first_acts[0], second_acts[0])
        out, sims = pl.pallas_call(
            write_out,
            out_shape=(
                jax.ShapeDtypeStruct((2, R, 2, hp, D, D), f32),
                jax.ShapeDtypeStruct((2, HEADS), f32),
            ),
            in_specs=[pl.BlockSpec(memory_space=pl.ANY)] * 2,
            out_specs=(pl.BlockSpec(memory_space=pltpu.MemorySpace.HBM),) * 2,
            scratch_shapes=[dma(2 * R + 1)],
            compiler_params=pltpu.CompilerParams(vmem_limit_bytes=1024 * 1024),
        )(out, sims)
        whitening = out.reshape(2, R * 2 * hp, D, D)[:, None, :HEADS]
        return whitening, sims[None]

    in_specs = (P("lay", "tok", None), P("lay", "tok", None))
    out_specs = (P(None, "lay", None, None, None), P("lay", None, None))
    return jax.shard_map(local, mesh=mesh, in_specs=in_specs, out_specs=out_specs, check_vma=False)
```
